256 devices in a mesh: dp: 64 (over z, y, core), cp: 4 (over x).
Axes of the slice: x: 4, y: 4, z: 8, core: 2. Of those that a mesh axis runs over, the one named last changes fastest.
Arguments:
- hidden: bfloat16 [64, 2048, 2048], P('dp', 'cp')
- positions: int32 [2048], P('cp')
- w_q: bfloat16 [2048, 2048], replicated
- w_k: bfloat16 [2048, 2048], replicated
- w_v: bfloat16 [2048, 2048], replicated
- w_o: bfloat16 [2048, 2048], replicated
Outputs:
- output 1: bfloat16 [64, 2048, 2048], P('dp', 'cp')
- output 2: float32 [16], replicated
- output 3: bfloat16 [2048, 2048], replicated
- output 4: bfloat16 [2048, 2048], replicated
All inputs are finite; a program needn't handle non-finite values.
Results may differ from the reference program's by a relative error of at most 0.00783462.
Values are sent between devices in bfloat16 or wider.
A program may use at most 768 MiB of HBM per device.

```python
import jax
import jax.numpy as jnp
from jax import lax

BATCH_SIZE = 64
SEQ_LEN = 2048
D_MODEL = 2048
NUM_HEADS = 16
QUERY_BLOCK = 64
HEAD_DIM = 128
TAU_CLIP = 100
ROPE_THETA = 50000


def rope_rotate(tensor, pos_ids):
    half_dim = HEAD_DIM // 2
    inv_freq = jnp.float32(ROPE_THETA) ** (-jnp.arange(half_dim, dtype=jnp.float32) * (2.0 / HEAD_DIM))
    angle = pos_ids.astype(jnp.float32)[:, None] * inv_freq[None, :]
    cos_t = jnp.cos(angle)[:, None, :]
    sin_t = jnp.sin(angle)[:, None, :]
    lead_half = tensor[..., :half_dim]
    tail_half = tensor[..., half_dim:]
    return jnp.concatenate([lead_half * cos_t - tail_half * sin_t, tail_half * cos_t + lead_half * sin_t], axis=-1)


def setup_inputs(seed: int = 0) -> dict:
    root_key = jax.random.key(seed)
    sub_keys = jax.random.split(root_key, 15)
    width = NUM_HEADS * HEAD_DIM
    gaps = jax.random.randint(sub_keys[0], (SEQ_LEN,), 1, 3)
    start_pos = jax.random.randint(sub_keys[1], (), 0, SEQ_LEN // 2 + 1)
    positions = (start_pos + jnp.cumsum(gaps) - 1).astype(jnp.int32)
    spike_row = jax.random.randint(sub_keys[2], (), 0, BATCH_SIZE)
    key_slot = jax.random.randint(sub_keys[3], (), 0, SEQ_LEN // 2)
    query_slot = jax.random.randint(sub_keys[4], (), SEQ_LEN // 2, SEQ_LEN)
    clip_heads = (jax.random.permutation(sub_keys[5], NUM_HEADS) < NUM_HEADS // 2).astype(jnp.float32)
    head_gain = jax.random.uniform(sub_keys[6], (NUM_HEADS,), jnp.float32, 1.0, 1.25)
    dir_query = jax.random.normal(sub_keys[7], (D_MODEL,), jnp.float32)
    dir_query = dir_query / jnp.sqrt(jnp.sum(dir_query * dir_query))
    dir_key = jax.random.normal(sub_keys[8], (D_MODEL,), jnp.float32)
    dir_key = dir_key / jnp.sqrt(jnp.sum(dir_key * dir_key))
    plant_q = jax.random.normal(sub_keys[9], (NUM_HEADS, HEAD_DIM), jnp.float32)
    plant_q = plant_q / jnp.sqrt(jnp.mean(plant_q * plant_q, axis=-1, keepdims=True))
    plant_q = plant_q * (4.0 * head_gain * clip_heads)[:, None] * D_MODEL ** -0.5
    delta = positions[query_slot] - positions[key_slot]
    plant_k = rope_rotate(plant_q[None], delta[None])[0]
    noise_scale = 1.5 * D_MODEL ** -0.5
    w_q = noise_scale * jax.random.normal(sub_keys[10], (D_MODEL, width), jnp.float32) + dir_query[:, None] * plant_q.reshape(width)[None, :]
    w_k = noise_scale * jax.random.normal(sub_keys[11], (D_MODEL, width), jnp.float32) + dir_key[:, None] * plant_k.reshape(width)[None, :]
    w_v = jax.random.normal(sub_keys[12], (D_MODEL, width), jnp.float32) * D_MODEL ** -0.5
    w_o = jax.random.normal(sub_keys[13], (width, D_MODEL), jnp.float32) * width ** -0.5
    hidden = jax.random.normal(sub_keys[14], (BATCH_SIZE, SEQ_LEN, D_MODEL), jnp.float32)
    spike_scale = jnp.sqrt(jnp.float32(D_MODEL))
    hidden = hidden.at[spike_row, query_slot].set(spike_scale * dir_query)
    hidden = hidden.at[spike_row, key_slot].set(spike_scale * dir_key)
    return {
        "hidden": hidden.astype(jnp.bfloat16),
        "positions": positions,
        "w_q": w_q.astype(jnp.bfloat16),
        "w_k": w_k.astype(jnp.bfloat16),
        "w_v": w_v.astype(jnp.bfloat16),
        "w_o": w_o.astype(jnp.bfloat16),
    }


def reference(hidden, positions, w_q, w_k, w_v, w_o):
    score_scale = HEAD_DIM ** -0.5
    n_blocks = SEQ_LEN // QUERY_BLOCK
    pos_blocks = positions.reshape(n_blocks, QUERY_BLOCK)
    head_shape = (SEQ_LEN, NUM_HEADS, HEAD_DIM)

    def one_row(row_in):
        q_all = rope_rotate(jnp.dot(row_in, w_q, preferred_element_type=jnp.float32).reshape(head_shape), positions).astype(jnp.bfloat16)
        k_all = rope_rotate(jnp.dot(row_in, w_k, preferred_element_type=jnp.float32).reshape(head_shape), positions).astype(jnp.bfloat16)
        v_all = jnp.dot(row_in, w_v, preferred_element_type=jnp.float32).astype(jnp.bfloat16).reshape(head_shape)
        k_wide = k_all.astype(jnp.float32)
        v_wide = v_all.astype(jnp.float32)
        q_blocks = q_all.reshape(n_blocks, QUERY_BLOCK, NUM_HEADS, HEAD_DIM)

        def one_block(block_in):
            q_blk, pos_blk = block_in
            scores = jnp.einsum("qhd,khd->hqk", q_blk.astype(jnp.float32), k_wide) * score_scale
            allowed = positions[None, None, :] <= pos_blk[None, :, None]
            scores = jnp.where(allowed, scores, -jnp.inf)
            block_max = jnp.max(scores, axis=(1, 2))
            prob_w = jax.nn.softmax(scores, axis=-1)
            attn_blk = jnp.einsum("hqk,khd->qhd", prob_w, v_wide)
            return attn_blk.astype(jnp.bfloat16), block_max

        attn_blocks, block_maxes = lax.map(one_block, (q_blocks, pos_blocks))
        attn_flat = attn_blocks.reshape(SEQ_LEN, NUM_HEADS * HEAD_DIM)
        row_out = jnp.dot(attn_flat, w_o, preferred_element_type=jnp.float32).astype(jnp.bfloat16)
        return row_out, jnp.max(block_maxes, axis=0)

    attn_out, row_maxes = lax.map(one_row, hidden)
    head_max = jnp.max(row_maxes, axis=0)
    factor = jnp.where(head_max > TAU_CLIP, jnp.sqrt(TAU_CLIP / head_max), 1.0)
    col_factor = jnp.repeat(factor, HEAD_DIM)
    w_q_new = (w_q.astype(jnp.float32) * col_factor[None, :]).astype(jnp.bfloat16)
    w_k_new = (w_k.astype(jnp.float32) * col_factor[None, :]).astype(jnp.bfloat16)
    return attn_out, head_max, w_q_new, w_k_new
```

```python
import functools

import jax
import jax.numpy as jnp
from jax import lax
from jax.experimental import pallas as pl
from jax.experimental.pallas import tpu as pltpu
from jax.sharding import PartitionSpec as P

HEAD_DIM = 128
TAU_CLIP = 100.0
ROPE_THETA = 50000.0
SCALE = HEAD_DIM ** -0.5
LOG2E = 1.4426950408889634
MESH = pl.DeviceIdType.MESH

PIECE = 512
HALF = 256
MODEL = 2048
COLS = 1024
HEADS = 8
OWN, FAR, NEAR, LAST = 0, 1, 2, 3
F32, BF16 = jnp.float32, jnp.bfloat16


def attend_kernel(hid, pos, freq, w_q, w_k, w_v, w_o, out, peak,
                  hbuf, wq, wk, wv, wo, qbuf, kbuf, vbuf, acc, run_max, run_sum, o_all, o_send, cos_t, sin_t, pos_all,
                  wsem, send, recv, psend, precv, osem):
    x = lax.axis_index("cp")
    d = lax.axis_index("dp")
    core = lax.rem(d, 2)
    home = core == x // 2
    away = core != x // 2
    partner = d + 1 - 2 * core
    pair = x + 1 - 2 * lax.rem(x, 2)
    far_x = 3 - x
    piece_of = (x, far_x, pair, 3 - pair)
    col0 = pl.multiple_of(core * COLS, COLS)

    def rows(kind, half):
        return pl.ds(pl.multiple_of(piece_of[kind] * PIECE + half * HALF, HALF), HALF)

    def remote(src, dst, s_sem, r_sem, dp, cp):
        return pltpu.make_async_remote_copy(src_ref=src, dst_ref=dst, send_sem=s_sem, recv_sem=r_sem,
                                            device_id={"dp": dp, "cp": cp}, device_id_type=MESH)

    w_copies = [pltpu.make_async_copy(src.at[:, pl.ds(col0, COLS)], dst, wsem.at[i])
                for i, (src, dst) in enumerate(((w_k, wk), (w_v, wv), (w_q, wq)))]
    w_copies.append(pltpu.make_async_copy(w_o, wo, wsem.at[3]))
    own_local = [pltpu.make_async_copy(hid.at[pl.ds(j * HALF, HALF), :], hbuf.at[rows(OWN, j), :], wsem.at[4 + j])
                 for j in range(2)]

    @pl.when(home)
    def _():
        for j in range(2):
            own_local[j].start()
    for copy in w_copies:
        copy.start()

    barrier = pltpu.get_barrier_semaphore()
    for k in range(1, 4):
        pl.semaphore_signal(barrier, inc=1, device_id={"dp": d, "cp": lax.rem(x + k, 4)}, device_id_type=MESH)
    pl.semaphore_signal(barrier, inc=1, device_id={"dp": partner, "cp": x}, device_id_type=MESH)
    pl.semaphore_wait(barrier, 4)

    def own_copy(j, to_pair):
        src = hid.at[pl.ds(j * HALF, HALF), :]
        dst = hbuf.at[rows(OWN, j), :]
        if to_pair:
            return remote(src, dst, send.at[j], recv.at[NEAR * 2 + j], d, pair)
        return remote(src, dst, send.at[2 + j], recv.at[OWN * 2 + j], partner, x)

    def away_copy(j):
        return remote(hid.at[pl.ds(j * HALF, HALF), :], hbuf.at[rows(OWN, j), :], send.at[12 + j], recv.at[FAR * 2 + j], d, far_x)

    def far_to_pair(j):
        return remote(hbuf.at[rows(FAR, j), :], hbuf.at[rows(FAR, j), :], send.at[4 + j], recv.at[LAST * 2 + j], d, pair)

    def to_partner(kind, j):
        return remote(hbuf.at[rows(kind, j), :], hbuf.at[rows(kind, j), :], send.at[4 + 2 * kind + j], recv.at[kind * 2 + j], partner, x)

    pos_copies = [remote(pos, pos_all.at[x], psend.at[k - 1], precv.at[k - 1], d, lax.rem(x + k, 4)) for k in range(1, 4)]
    for copy in pos_copies:
        copy.start()

    @pl.when(home)
    def _():
        @pl.when(x != 3)
        def _():
            for j in range(2):
                own_copy(j, True).start()
        for j in range(2):
            own_copy(j, False).start()

    @pl.when(away)
    def _():
        for j in range(2):
            away_copy(j).start()

    for copy in pos_copies:
        copy.wait_recv()

    def tables(kind):
        piece = piece_of[kind]
        row_i = lax.broadcasted_iota(jnp.int32, (128, 128), 0)
        col_i = lax.broadcasted_iota(jnp.int32, (128, 128), 1)
        sign = jnp.where(lax.broadcasted_iota(jnp.int32, (1, 128), 1) < 64, -1.0, 1.0)

        def block(b, carry):
            if kind == OWN:
                line = pos[pl.ds(b, 1), :]
            else:
                line = pos_all[pl.ds(piece, 1), pl.ds(b, 1), :].reshape(1, 128)
            line = jnp.broadcast_to(line.astype(F32), (128, 128))
            column = jnp.sum(jnp.where(row_i == col_i, line, 0.0), axis=1, keepdims=True)
            angle = column * freq[...]
            at = pl.ds(pl.multiple_of(piece * PIECE + b * 128, 128), 128)
            cos_t[at, :] = jnp.cos(angle)
            sin_t[at, :] = jnp.sin(angle) * sign
            return carry

        lax.fori_loop(0, 4, block, 0)

    def rotate(t, cos_v, sin_v):
        return (t * cos_v + pltpu.roll(t, 64, 1) * sin_v).astype(BF16)

    def project(kind, half, with_q):
        at = rows(kind, half)
        cos_v, sin_v = cos_t[at, :], sin_t[at, :]
        slot_rows = pl.ds(half * HALF, HALF)

        def block(n, carry):
            cols = pl.ds(pl.multiple_of(n * 256, 256), 256)
            h = hbuf[at, :]
            k2 = jnp.dot(h, wk[:, cols], preferred_element_type=F32)
            v2 = jnp.dot(h, wv[:, cols], preferred_element_type=F32)
            kbuf[at, cols] = jnp.concatenate([rotate(k2[:, :128], cos_v, sin_v), rotate(k2[:, 128:], cos_v, sin_v)], axis=1)
            vbuf[at, cols] = v2.astype(BF16)
            if with_q:
                q2 = jnp.dot(h, wq[:, cols], preferred_element_type=F32)
                qbuf[kind, slot_rows, cols] = jnp.concatenate(
                    [rotate(q2[:, :128], cos_v, sin_v), rotate(q2[:, 128:], cos_v, sin_v)], axis=1)
            return carry

        lax.fori_loop(0, 4, block, 0)

    def tile(slot, piece, diagonal):
        key0 = pl.multiple_of(piece * PIECE, PIECE)

        def head(h, carry):
            cols = pl.ds(pl.multiple_of(h * HEAD_DIM, HEAD_DIM), HEAD_DIM)
            for qb in range(2):
                n_keys = HALF * (qb + 1) if diagonal else PIECE
                at = pl.ds(qb * HALF, HALF)
                k = kbuf[pl.ds(key0, n_keys), cols]
                v = vbuf[pl.ds(key0, n_keys), cols]
                s = lax.dot_general(qbuf[slot, at, cols], k, (((1,), (1,)), ((), ())), preferred_element_type=F32)
                if diagonal:
                    q_i = lax.broadcasted_iota(jnp.int32, (HALF, n_keys), 0) + qb * HALF
                    s = jnp.where(q_i >= lax.broadcasted_iota(jnp.int32, (HALF, n_keys), 1), s, -jnp.inf)
                top = jnp.max(s, axis=1, keepdims=True)
                if diagonal:
                    new = jnp.broadcast_to(top, (HALF, 128))
                else:
                    old = run_max[slot, h, at, :]
                    new = jnp.maximum(old, top)
                p = jnp.exp2((s - jnp.concatenate([new] * (n_keys // 128), axis=1)) * (SCALE * LOG2E))
                total = jnp.broadcast_to(jnp.sum(p, axis=1, keepdims=True), (HALF, 128))
                part = jnp.dot(p.astype(BF16), v, preferred_element_type=F32)
                if not diagonal:
                    fade = jnp.exp2((old - new) * (SCALE * LOG2E))
                    total = total + run_sum[slot, h, at, :] * fade
                    part = part + acc[slot, at, cols] * fade
                run_max[slot, h, at, :] = new
                run_sum[slot, h, at, :] = total
                acc[slot, at, cols] = part
            return carry

        lax.fori_loop(0, HEADS, head, 0)

    def arrive(kind, j):
        @pl.when(home)
        def _():
            if kind == OWN:
                own_local[j].wait()
            else:
                away_copy(j).wait_recv() if kind == FAR else own_copy(j, True).wait_recv() if kind == NEAR else far_to_pair(j).wait_recv()
                if kind == FAR:
                    @pl.when(x != 0)
                    def _():
                        far_to_pair(j).start()
                to_partner(kind, j).start()

        @pl.when(away)
        def _():
            if kind == OWN:
                own_copy(j, False).wait_recv()
            else:
                to_partner(kind, j).wait_recv()

    w_copies[0].wait()
    tables(OWN)
    w_copies[1].wait()
    w_copies[2].wait()
    for j in range(2):
        arrive(OWN, j)
        project(OWN, j, True)
    tile(OWN, x, True)
    tables(FAR)
    tables(NEAR)
    tables(LAST)
    for j in range(2):
        arrive(FAR, j)
        project(FAR, j, True)

        @pl.when(x != 2)
        def _():
            arrive(NEAR, j)
            project(NEAR, j, False)
    tile(FAR, far_x, True)
    later = jnp.where(x < 2, FAR, OWN)
    tile(later, jnp.where(x < 2, x, far_x), False)

    @pl.when(x <= 1)
    def _():
        tile(FAR, pair, False)

    @pl.when((x == 1) | (x == 3))
    def _():
        tile(OWN, pair, False)

    @pl.when(x != 1)
    def _():
        for j in range(2):
            arrive(LAST, j)
            project(LAST, j, False)

    @pl.when((x == 0) | (x == 2))
    def _():
        tile(FAR, 3 - pair, False)

    @pl.when(x >= 2)
    def _():
        tile(OWN, 3 - pair, False)

    keep = jnp.where(home, OWN, FAR)
    give = 1 - keep

    def finish(slot, dst):
        def head(h, carry):
            cols = pl.ds(pl.multiple_of(h * HEAD_DIM, HEAD_DIM), HEAD_DIM)
            dst[:, cols] = (acc[slot, :, cols] / run_sum[slot, h, :, :]).astype(BF16)
            return carry
        lax.fori_loop(0, HEADS, head, 0)

    exchange = remote(o_send, o_all.at[core], osem.at[0], osem.at[1], partner, x)
    finish(give, o_send)
    exchange.start()
    finish(keep, o_all.at[core])

    peak[...] = jnp.full(peak.shape, -jnp.inf, F32)

    def head_top(h, carry):
        top = jnp.maximum(jnp.max(run_max[0, h, :, :], axis=0, keepdims=True), jnp.max(run_max[1, h, :, :], axis=0, keepdims=True))
        peak[pl.ds(core * HEADS + h, 1), :] = top * SCALE
        return carry

    lax.fori_loop(0, HEADS, head_top, 0)
    w_copies[3].wait()
    exchange.wait_recv()

    def out_block(n, carry):
        cols = pl.ds(pl.multiple_of(n * 256, 256), 256)
        out[:, cols] = (jnp.dot(o_all[0], wo[:COLS, cols], preferred_element_type=F32)
                        + jnp.dot(o_all[1], wo[COLS:, cols], preferred_element_type=F32)).astype(BF16)
        return carry

    lax.fori_loop(0, MODEL // 256, out_block, 0)

    exchange.wait_send()
    for copy in pos_copies:
        copy.wait_send()

    @pl.when(away)
    def _():
        for j in range(2):
            away_copy(j).wait_send()

    @pl.when(home)
    def _():
        for j in range(2):
            own_copy(j, False).wait_send()
            to_partner(FAR, j).wait_send()

        @pl.when(x != 3)
        def _():
            for j in range(2):
                own_copy(j, True).wait_send()

        @pl.when(x != 0)
        def _():
            for j in range(2):
                far_to_pair(j).wait_send()

        @pl.when(x != 2)
        def _():
            for j in range(2):
                to_partner(NEAR, j).wait_send()

        @pl.when(x != 1)
        def _():
            for j in range(2):
                to_partner(LAST, j).wait_send()


def attend(hid, pos, freq, w_q, w_k, w_v, w_o):
    any_spec = pl.BlockSpec(memory_space=pl.ANY)
    vmem = pl.BlockSpec(memory_space=pltpu.VMEM)
    return pl.pallas_call(
        attend_kernel,
        name="attend",
        out_shape=[jax.ShapeDtypeStruct((PIECE, MODEL), BF16), jax.ShapeDtypeStruct((2 * HEADS, 128), F32)],
        in_specs=[any_spec, vmem, vmem, any_spec, any_spec, any_spec, any_spec],
        out_specs=[vmem, vmem],
        scratch_shapes=[
            pltpu.VMEM((4 * PIECE, MODEL), BF16),
            pltpu.VMEM((MODEL, COLS), BF16), pltpu.VMEM((MODEL, COLS), BF16), pltpu.VMEM((MODEL, COLS), BF16),
            pltpu.VMEM((MODEL, MODEL), BF16),
            pltpu.VMEM((2, PIECE, COLS), BF16), pltpu.VMEM((4 * PIECE, COLS), BF16), pltpu.VMEM((4 * PIECE, COLS), BF16),
            pltpu.VMEM((2, PIECE, COLS), F32), pltpu.VMEM((2, HEADS, PIECE, 128), F32), pltpu.VMEM((2, HEADS, PIECE, 128), F32),
            pltpu.VMEM((2, PIECE, COLS), BF16), pltpu.VMEM((PIECE, COLS), BF16),
            pltpu.VMEM((4 * PIECE, 128), F32), pltpu.VMEM((4 * PIECE, 128), F32), pltpu.VMEM((4, 8, 128), jnp.int32),
            pltpu.SemaphoreType.DMA((6,)), pltpu.SemaphoreType.DMA((14,)), pltpu.SemaphoreType.DMA((8,)),
            pltpu.SemaphoreType.DMA((3,)), pltpu.SemaphoreType.DMA((3,)), pltpu.SemaphoreType.DMA((2,)),
        ],
        compiler_params=pltpu.CompilerParams(collective_id=0, has_side_effects=True, vmem_limit_bytes=67043328),
        cost_estimate=pl.CostEstimate(flops=31_000_000_000, bytes_accessed=26_000_000, transcendentals=11_000_000),
    )(hid, pos, freq, w_q, w_k, w_v, w_o)


def peak_kernel(sizes, peak, best, cur, slots, send, recv):
    n_z, n_y, n_x = sizes
    x = lax.axis_index("cp")
    d = lax.axis_index("dp")
    core, y, z = lax.rem(d, 2), lax.rem(d // 2, n_y), d // (2 * n_y)
    rounds = [
        [(d + 1 - 2 * core, x)],
        [(d, lax.rem(x + k, n_x)) for k in range(1, n_x)],
        [((z * n_y + lax.rem(y + k, n_y)) * 2 + core, x) for k in range(1, n_y)],
        [((lax.rem(z + k, n_z) * n_y + y) * 2 + core, x) for k in range(1, n_z)],
    ]
    barrier = pltpu.get_barrier_semaphore()
    total = 0
    for peers in rounds:
        for dp, cp in peers:
            pl.semaphore_signal(barrier, inc=1, device_id={"dp": dp, "cp": cp}, device_id_type=MESH)
            total += 1
    cur[0] = peak[...]
    pl.semaphore_wait(barrier, total)
    index = 0
    copies = []
    for r, peers in enumerate(rounds):
        batch = []
        for dp, cp in peers:
            batch.append((index, pltpu.make_async_remote_copy(
                src_ref=cur.at[r], dst_ref=slots.at[index], send_sem=send.at[index], recv_sem=recv.at[index],
                device_id={"dp": dp, "cp": cp}, device_id_type=MESH)))
            index += 1
        for _, copy in batch:
            copy.start()
        value = cur[r]
        for i, copy in batch:
            copy.wait_recv()
            value = jnp.maximum(value, slots[i])
        if r + 1 < len(rounds):
            cur[r + 1] = value
        else:
            best[...] = value
        copies += batch
    for _, copy in copies:
        copy.wait_send()


def global_peak(peak, sizes):
    n_copies = 1 + sum(n - 1 for n in sizes)
    vmem = pl.BlockSpec(memory_space=pltpu.VMEM)
    shape = peak.shape
    return pl.pallas_call(
        functools.partial(peak_kernel, sizes),
        name="global_peak",
        out_shape=jax.ShapeDtypeStruct(shape, F32),
        in_specs=[vmem], out_specs=vmem,
        scratch_shapes=[pltpu.VMEM((4,) + shape, F32), pltpu.VMEM((n_copies,) + shape, F32),
                        pltpu.SemaphoreType.DMA((n_copies,)), pltpu.SemaphoreType.DMA((n_copies,))],
        compiler_params=pltpu.CompilerParams(collective_id=1, has_side_effects=True),
        cost_estimate=pl.CostEstimate(flops=10_000_000, bytes_accessed=8192, transcendentals=0),
    )(peak)


def clip_weights(head_max, w_q, w_k):
    factor = jnp.where(head_max > TAU_CLIP, jnp.sqrt(TAU_CLIP / head_max), 1.0)
    col_factor = jnp.repeat(factor, HEAD_DIM)[None, :]
    return (w_q.astype(F32) * col_factor).astype(BF16), (w_k.astype(F32) * col_factor).astype(BF16)


def solution(mesh):
    cp_size, dp_size = mesh.shape["cp"], mesh.shape["dp"]
    sizes = (dp_size // 8, 4, cp_size)
    swap = []
    for quad in range(dp_size // 2):
        for x in range(cp_size):
            src_dp = 2 * quad + 1 - x // 2
            dst_x = cp_size - 1 - x
            dst_dp = 2 * quad + 1 - dst_x // 2
            swap.append((src_dp * cp_size + x, dst_dp * cp_size + dst_x))

    def device_body(hidden, pos_ids, w_q, w_k, w_v, w_o):
        half_dim = HEAD_DIM // 2
        inv_freq = jnp.float32(ROPE_THETA) ** (-jnp.arange(half_dim, dtype=F32) * (2.0 / HEAD_DIM))
        freq = jnp.concatenate([inv_freq, inv_freq])[None, :]
        pos = jnp.pad(pos_ids.reshape(4, 128), ((0, 4), (0, 0)))
        out, peak = attend(hidden[0], pos, freq, w_q, w_k, w_v, w_o)
        swapped = lax.ppermute(out, ("dp", "cp"), swap)
        head_max = global_peak(peak, sizes)[:, 0]
        w_q_new, w_k_new = clip_weights(head_max, w_q, w_k)
        home = lax.rem(lax.axis_index("dp"), 2) == lax.axis_index("cp") // 2
        return jnp.where(home, out, swapped)[None], head_max, w_q_new, w_k_new

    return jax.shard_map(
        device_body,
        mesh=mesh,
        in_specs=(P("dp", "cp", None), P("cp"), P(None, None), P(None, None), P(None, None), P(None, None)),
        out_specs=(P("dp", "cp", None), P(None), P(None, None), P(None, None)),
        check_vma=False,
    )
```

```python
import functools

import jax
import jax.numpy as jnp
import numpy as np
from jax import lax
from jax.experimental import pallas as pl
from jax.experimental.pallas import tpu as pltpu
from jax.sharding import PartitionSpec as P

HEAD_DIM = 128
TAU_CLIP = 100.0
ROPE_THETA = 50000.0
SCALE = HEAD_DIM ** -0.5
LOG2E = 1.4426950408889634
MESH = pl.DeviceIdType.MESH

PIECE = 512
HALF = 256
MODEL = 2048
COLS = 1024
HEADS = 8
OWN, FAR, NEAR, LAST = 0, 1, 2, 3
TABLE_OF = (0, 0, 1, 0)
F32, BF16 = jnp.float32, jnp.bfloat16


def attend_kernel(hid, pos, freq, w_q, w_k, w_v, w_o, out, peak,
                  hbuf, wq, wk, wv, wo, qbuf, kbuf, vbuf, acc, run_max, run_sum, o_all, cos_t, sin_t, pos_all,
                  bias, top_all, wsem, send, recv, psend, precv, osem, tsend, trecv):
    x = lax.axis_index("cp")
    d = lax.axis_index("dp")
    core = lax.rem(d, 2)
    home = core == x // 2
    away = core != x // 2
    partner = d + 1 - 2 * core
    pair = x + 1 - 2 * lax.rem(x, 2)
    far_x = 3 - x
    piece_of = (x, far_x, pair, 3 - pair)
    col0 = pl.multiple_of(core * COLS, COLS)

    def rows(kind, half):
        return pl.ds(pl.multiple_of(piece_of[kind] * PIECE + half * HALF, HALF), HALF)

    def remote(src, dst, s_sem, r_sem, dp, cp):
        return pltpu.make_async_remote_copy(src_ref=src, dst_ref=dst, send_sem=s_sem, recv_sem=r_sem,
                                            device_id={"dp": dp, "cp": cp}, device_id_type=MESH)

    w_copies = [pltpu.make_async_copy(src.at[:, pl.ds(col0, COLS)], dst, wsem.at[i])
                for i, (src, dst) in enumerate(((w_k, wk), (w_v, wv), (w_q, wq)))]
    w_copies.append(pltpu.make_async_copy(w_o.at[:, pl.ds(COLS, COLS)], wo, wsem.at[3]))
    wo_low = pltpu.make_async_copy(w_o.at[:, pl.ds(0, COLS)], wq, wsem.at[6])

    def half_rows(j):
        return pl.ds(pl.multiple_of(j * HALF, HALF), HALF)

    def own_local(j):
        return pltpu.make_async_copy(hid.at[half_rows(j), :], hbuf.at[rows(OWN, j), :], wsem.at[4 + j])

    @pl.when(home)
    def _():
        for j in range(2):
            own_local(j).start()
    for copy in w_copies:
        copy.start()

    barrier = pltpu.get_barrier_semaphore()
    for k in range(1, 4):
        pl.semaphore_signal(barrier, inc=1, device_id={"dp": d, "cp": lax.rem(x + k, 4)}, device_id_type=MESH)
    pl.semaphore_signal(barrier, inc=1, device_id={"dp": partner, "cp": x}, device_id_type=MESH)
    pl.semaphore_wait(barrier, 4)

    def own_copy(j, to_pair):
        src = hid.at[half_rows(j), :]
        dst = hbuf.at[rows(OWN, j), :]
        if to_pair:
            return remote(src, dst, send.at[j], recv.at[NEAR * 2 + j], d, pair)
        return remote(src, dst, send.at[2 + j], recv.at[OWN * 2 + j], partner, x)

    def away_copy(j):
        return remote(hid.at[half_rows(j), :], hbuf.at[rows(OWN, j), :], send.at[12 + j], recv.at[FAR * 2 + j], d, far_x)

    def far_to_pair(j):
        return remote(hbuf.at[rows(FAR, j), :], hbuf.at[rows(FAR, j), :], send.at[4 + j], recv.at[LAST * 2 + j], d, pair)

    def to_partner(kind, j):
        return remote(hbuf.at[rows(kind, j), :], hbuf.at[rows(kind, j), :], send.at[4 + 2 * kind + j], recv.at[kind * 2 + j], partner, x)

    pos_copies = [remote(pos, pos_all.at[x], psend.at[k - 1], precv.at[k - 1], d, lax.rem(x + k, 4)) for k in range(1, 4)]
    for copy in pos_copies:
        copy.start()

    @pl.when(home)
    def _():
        @pl.when(x != 3)
        def _():
            for j in range(2):
                own_copy(j, True).start()
        for j in range(2):
            own_copy(j, False).start()

    @pl.when(away)
    def _():
        for j in range(2):
            away_copy(j).start()

    def tables(kind):
        piece = piece_of[kind]
        row_i = lax.broadcasted_iota(jnp.int32, (64, 128), 0)
        col_i = lax.broadcasted_iota(jnp.int32, (64, 128), 1)
        low = col_i < 64

        def block(b, carry):
            if kind == OWN:
                line = pos[pl.ds(b, 1), :]
            else:
                line = pos_all[pl.ds(piece, 1), pl.ds(b, 1), :].reshape(1, 128)
            line = jnp.broadcast_to(line.astype(F32), (64, 128))
            first = jnp.sum(jnp.where(row_i == col_i, line, 0.0), axis=1, keepdims=True)
            second = jnp.sum(jnp.where(row_i + 64 == col_i, line, 0.0), axis=1, keepdims=True)
            angle = jnp.where(low, first, second) * freq[...]
            cos_a, sin_a = jnp.cos(angle), jnp.sin(angle)
            cos_r, sin_r = pltpu.roll(cos_a, 64, 1), pltpu.roll(sin_a, 64, 1)
            at = pl.multiple_of(TABLE_OF[kind] * PIECE + b * 128, 128)
            cos_t[pl.ds(at, 64), :] = jnp.where(low, cos_a, cos_r)
            cos_t[pl.ds(at + 64, 64), :] = jnp.where(low, cos_r, cos_a)
            sin_t[pl.ds(at, 64), :] = jnp.where(low, -sin_a, sin_r)
            sin_t[pl.ds(at + 64, 64), :] = jnp.where(low, -sin_r, sin_a)
            return carry

        lax.fori_loop(0, 4, block, 0)

    def rotate(t, cos_v, sin_v):
        parts = []
        for h in range(HEADS):
            u = t[:, h * HEAD_DIM:(h + 1) * HEAD_DIM]
            parts.append((u * cos_v + pltpu.roll(u, 64, 1) * sin_v).astype(BF16))
        return jnp.concatenate(parts, axis=1)

    def project(kind, half, with_q):
        at = rows(kind, half)
        table = pl.ds(pl.multiple_of(TABLE_OF[kind] * PIECE + half * HALF, HALF), HALF)
        cos_v, sin_v = cos_t[table, :], sin_t[table, :]
        h = hbuf[at, :]
        kbuf[at, :] = rotate(jnp.dot(h, wk[...], preferred_element_type=F32), cos_v, sin_v)
        vbuf[at, :] = jnp.dot(h, wv[...], preferred_element_type=F32).astype(BF16)
        if with_q:
            q_at = pl.ds(pl.multiple_of(half * HALF, HALF), HALF)
            qbuf[kind, q_at, :] = rotate(jnp.dot(h, wq[...], preferred_element_type=F32), cos_v, sin_v)

    def tile(slot, piece, diagonal):
        key0 = pl.multiple_of(piece * PIECE, PIECE)
        units = [(h, qb) for h in range(HEADS) for qb in range(2)]

        def scores(h, qb):
            n_keys = HALF * (qb + 1) if diagonal else PIECE
            cols = pl.ds(h * HEAD_DIM, HEAD_DIM)
            s = lax.dot_general(qbuf[slot, pl.ds(qb * HALF, HALF), cols], kbuf[pl.ds(key0, n_keys), cols],
                                (((1,), (1,)), ((), ())), preferred_element_type=F32)
            if diagonal:
                last = s[:, n_keys - HALF:] + bias[...]
                s = last if qb == 0 else jnp.concatenate([s[:, :n_keys - HALF], last], axis=1)
            return s

        results = []
        s = scores(*units[0])
        for i, (h, qb) in enumerate(units):
            s_next = scores(*units[i + 1]) if i + 1 < len(units) else None
            at = pl.ds(qb * HALF, HALF)
            n_keys = s.shape[1]
            top = jnp.max(s, axis=1, keepdims=True)
            old = None if diagonal else run_max[slot, h, at, :]
            new = jnp.broadcast_to(top, (HALF, 128)) if diagonal else jnp.maximum(old, top)
            p = jnp.exp2((s - jnp.concatenate([new] * (n_keys // 128), axis=1)) * (SCALE * LOG2E))
            total = p[:, :128]
            for g in range(1, n_keys // 128):
                total = total + p[:, g * 128:(g + 1) * 128]
            part = jnp.dot(p.astype(BF16), vbuf[pl.ds(key0, n_keys), pl.ds(h * HEAD_DIM, HEAD_DIM)],
                           preferred_element_type=F32)
            results.append((old, new, total, part))
            s = s_next
        for (h, qb), (old, new, total, part) in zip(units, results):
            at, cols = pl.ds(qb * HALF, HALF), pl.ds(h * HEAD_DIM, HEAD_DIM)
            if not diagonal:
                fade = jnp.exp2((old - new) * (SCALE * LOG2E))
                total = total + run_sum[slot, h, at, :] * fade
                part = part + acc[slot, at, cols] * fade
            run_max[slot, h, at, :] = new
            run_sum[slot, h, at, :] = total
            acc[slot, at, cols] = part

    def arrive(kind, j):
        @pl.when(home)
        def _():
            if kind == OWN:
                own_local(j).wait()
            else:
                away_copy(j).wait_recv() if kind == FAR else own_copy(j, True).wait_recv() if kind == NEAR else far_to_pair(j).wait_recv()
                if kind == FAR:
                    @pl.when(x != 0)
                    def _():
                        far_to_pair(j).start()
                to_partner(kind, j).start()

        @pl.when(away)
        def _():
            if kind == OWN:
                own_copy(j, False).wait_recv()
            else:
                to_partner(kind, j).wait_recv()

    bias[...] = jnp.where(lax.broadcasted_iota(jnp.int32, (HALF, HALF), 0) >= lax.broadcasted_iota(jnp.int32, (HALF, HALF), 1),
                          0.0, -jnp.inf)
    tables(OWN)
    for i in range(3):
        w_copies[i].wait()

    def own_half(j, carry):
        arrive(OWN, j)
        project(OWN, j, True)
        return carry

    lax.fori_loop(0, 2, own_half, 0)
    for copy in pos_copies:
        copy.wait_recv()
    tables(FAR)
    tables(NEAR)

    def far_half(j, carry):
        arrive(FAR, j)
        project(FAR, j, True)

        @pl.when(x != 2)
        def _():
            arrive(NEAR, j)
            project(NEAR, j, False)
        return carry

    lax.fori_loop(0, 2, far_half, 0)
    wo_low.start()
    tables(LAST)

    def diagonal_tile(slot, carry):
        tile(slot, jnp.where(slot == OWN, x, far_x), True)
        return carry

    lax.fori_loop(0, 2, diagonal_tile, 0)

    later = jnp.where(x < 2, FAR, OWN)

    def near_tile(i, carry):
        slot = jnp.where(i == 0, later, i - 1)
        piece = jnp.where(i == 0, jnp.minimum(x, far_x), pair)

        @pl.when((i == 0) | ((i == 1) & (lax.rem(x, 2) == 1)) | ((i == 2) & (x < 2)))
        def _():
            tile(slot, piece, False)
        return carry

    lax.fori_loop(0, 3, near_tile, 0)

    exchange = remote(qbuf.at[jnp.where(home, FAR, OWN)], o_all.at[core], osem.at[0], osem.at[1], partner, x)

    own_rows = pl.ds(pl.multiple_of(x * PIECE, PIECE), PIECE)

    def out_copy(part):
        cols = pl.ds(part * COLS, COLS)
        return pltpu.make_async_copy(hbuf.at[own_rows, cols], out.at[:, cols], wsem.at[7 + part])

    def section(slot):
        mine = (home & (slot == OWN)) | (away & (slot == FAR))

        def head(h, carry):
            cols = pl.ds(pl.multiple_of(h * HEAD_DIM, HEAD_DIM), HEAD_DIM)
            total = jnp.sum(run_sum[slot, h, :, :], axis=1, keepdims=True)
            value = (acc[slot, :, cols] / total).astype(BF16)

            @pl.when(mine)
            def _():
                o_all[core, :, cols] = value

            @pl.when(jnp.logical_not(mine))
            def _():
                qbuf[slot, :, cols] = value
            return carry

        lax.fori_loop(0, HEADS, head, 0)

        @pl.when(jnp.logical_not(mine))
        def _():
            exchange.start()

        @pl.when(mine)
        def _():
            exchange.wait_recv()

            for part, w in enumerate((wq, wo)):
                def out_block(n, carry):
                    cols = pl.ds(pl.multiple_of(n * 512, 512), 512)
                    value = (jnp.dot(o_all[0], w[:COLS, cols], preferred_element_type=F32)
                             + jnp.dot(o_all[1], w[COLS:, cols], preferred_element_type=F32))
                    hbuf[own_rows, pl.ds(pl.multiple_of(part * COLS + n * 512, 512), 512)] = value.astype(BF16)
                    return carry

                lax.fori_loop(0, COLS // 512, out_block, 0)
                out_copy(part).start()

    w_copies[3].wait()
    wo_low.wait()
    outer = (x == 0) | (x == 3)

    @pl.when(outer)
    def _():
        section(1 - later)

    @pl.when(x != 1)
    def _():
        def last_half(j, carry):
            arrive(LAST, j)
            project(LAST, j, False)
            return carry
        lax.fori_loop(0, 2, last_half, 0)

    def last_tile(slot, carry):
        @pl.when(((slot == OWN) & (x >= 2)) | ((slot == FAR) & (lax.rem(x, 2) == 0)))
        def _():
            tile(slot, 3 - pair, False)
        return carry

    lax.fori_loop(0, 2, last_tile, 0)

    top_all[0] = jnp.full((2 * HEADS, 128), -jnp.inf, F32)

    def head_top(h, carry):
        top = jnp.maximum(jnp.max(run_max[0, h, :, :], axis=0, keepdims=True), jnp.max(run_max[1, h, :, :], axis=0, keepdims=True))
        top_all[0, pl.ds(core * HEADS + h, 1), :] = top * SCALE
        return carry

    lax.fori_loop(0, HEADS, head_top, 0)
    top_copies = [remote(top_all.at[0], top_all.at[k], tsend.at[k - 1], trecv.at[k - 1], d, lax.rem(x + k, 4)) for k in range(1, 4)]
    for copy in top_copies:
        copy.start()

    def end_section(i, carry):
        section(jnp.where(i == 0, 1 - later, later))
        return carry

    lax.fori_loop(jnp.where(outer, 1, 0), 2, end_section, 0)

    best = top_all[0]
    for k, copy in enumerate(top_copies):
        copy.wait_recv()
        best = jnp.maximum(best, top_all[k + 1])
    peak[...] = best
    for copy in top_copies:
        copy.wait_send()

    for part in range(2):
        out_copy(part).wait()

    exchange.wait_send()
    for copy in pos_copies:
        copy.wait_send()

    @pl.when(away)
    def _():
        for j in range(2):
            away_copy(j).wait_send()

    @pl.when(home)
    def _():
        for j in range(2):
            own_copy(j, False).wait_send()
            to_partner(FAR, j).wait_send()

        @pl.when(x != 3)
        def _():
            for j in range(2):
                own_copy(j, True).wait_send()

        @pl.when(x != 0)
        def _():
            for j in range(2):
                far_to_pair(j).wait_send()

        @pl.when(x != 2)
        def _():
            for j in range(2):
                to_partner(NEAR, j).wait_send()

        @pl.when(x != 1)
        def _():
            for j in range(2):
                to_partner(LAST, j).wait_send()


def attend(hid, pos, freq, w_q, w_k, w_v, w_o):
    any_spec = pl.BlockSpec(memory_space=pl.ANY)
    vmem = pl.BlockSpec(memory_space=pltpu.VMEM)
    return pl.pallas_call(
        attend_kernel,
        name="attend",
        out_shape=[jax.ShapeDtypeStruct((PIECE, MODEL), BF16), jax.ShapeDtypeStruct((2 * HEADS, 128), F32)],
        in_specs=[any_spec, vmem, vmem, any_spec, any_spec, any_spec, any_spec],
        out_specs=[any_spec, vmem],
        scratch_shapes=[
            pltpu.VMEM((4 * PIECE, MODEL), BF16),
            pltpu.VMEM((MODEL, COLS), BF16), pltpu.VMEM((MODEL, COLS), BF16), pltpu.VMEM((MODEL, COLS), BF16),
            pltpu.VMEM((MODEL, COLS), BF16),
            pltpu.VMEM((2, PIECE, COLS), BF16), pltpu.VMEM((4 * PIECE, COLS), BF16), pltpu.VMEM((4 * PIECE, COLS), BF16),
            pltpu.VMEM((2, PIECE, COLS), F32), pltpu.VMEM((2, HEADS, PIECE, 128), F32), pltpu.VMEM((2, HEADS, PIECE, 128), F32),
            pltpu.VMEM((2, PIECE, COLS), BF16),
            pltpu.VMEM((2 * PIECE, 128), F32), pltpu.VMEM((2 * PIECE, 128), F32), pltpu.VMEM((4, 4, 128), jnp.int32),
            pltpu.VMEM((HALF, HALF), F32), pltpu.VMEM((4, 2 * HEADS, 128), F32),
            pltpu.SemaphoreType.DMA((9,)), pltpu.SemaphoreType.DMA((14,)), pltpu.SemaphoreType.DMA((8,)),
            pltpu.SemaphoreType.DMA((3,)), pltpu.SemaphoreType.DMA((3,)), pltpu.SemaphoreType.DMA((2,)),
            pltpu.SemaphoreType.DMA((3,)), pltpu.SemaphoreType.DMA((3,)),
        ],
        compiler_params=pltpu.CompilerParams(collective_id=0, has_side_effects=True, vmem_limit_bytes=67043328),
        cost_estimate=pl.CostEstimate(flops=31_000_000_000, bytes_accessed=26_000_000, transcendentals=11_000_000),
    )(hid, pos, freq, w_q, w_k, w_v, w_o)


def peak_kernel(sizes, peak, best, cur, slots, send, recv):
    n_z, n_y = sizes
    x = lax.axis_index("cp")
    d = lax.axis_index("dp")
    core, y, z = lax.rem(d, 2), lax.rem(d // 2, n_y), d // (2 * n_y)
    rounds = [
        [(d + 1 - 2 * core, x)],
        [((z * n_y + lax.rem(y + k, n_y)) * 2 + core, x) for k in range(1, n_y)],
        [((lax.rem(z + k, n_z) * n_y + y) * 2 + core, x) for k in range(1, n_z)],
    ]
    barrier = pltpu.get_barrier_semaphore()
    total = 0
    for peers in rounds:
        for dp, cp in peers:
            pl.semaphore_signal(barrier, inc=1, device_id={"dp": dp, "cp": cp}, device_id_type=MESH)
            total += 1
    cur[0] = peak[...]
    pl.semaphore_wait(barrier, total)
    index = 0
    copies = []
    for r, peers in enumerate(rounds):
        batch = []
        for dp, cp in peers:
            batch.append((index, pltpu.make_async_remote_copy(
                src_ref=cur.at[r], dst_ref=slots.at[index], send_sem=send.at[index], recv_sem=recv.at[index],
                device_id={"dp": dp, "cp": cp}, device_id_type=MESH)))
            index += 1
        for _, copy in batch:
            copy.start()
        value = cur[r]
        for i, copy in batch:
            copy.wait_recv()
            value = jnp.maximum(value, slots[i])
        if r + 1 < len(rounds):
            cur[r + 1] = value
        else:
            best[...] = value
        copies += batch
    for _, copy in copies:
        copy.wait_send()


def global_peak(peak, sizes):
    n_copies = 1 + sum(n - 1 for n in sizes)
    vmem = pl.BlockSpec(memory_space=pltpu.VMEM)
    shape = peak.shape
    return pl.pallas_call(
        functools.partial(peak_kernel, sizes),
        name="global_peak",
        out_shape=jax.ShapeDtypeStruct(shape, F32),
        in_specs=[vmem], out_specs=vmem,
        scratch_shapes=[pltpu.VMEM((3,) + shape, F32), pltpu.VMEM((n_copies,) + shape, F32),
                        pltpu.SemaphoreType.DMA((n_copies,)), pltpu.SemaphoreType.DMA((n_copies,))],
        compiler_params=pltpu.CompilerParams(collective_id=1, has_side_effects=True),
        cost_estimate=pl.CostEstimate(flops=10_000_000, bytes_accessed=8192, transcendentals=0),
    )(peak)


def clip_weights(head_max, w_q, w_k):
    factor = jnp.where(head_max > TAU_CLIP, jnp.sqrt(TAU_CLIP / head_max), 1.0)
    col_factor = jnp.repeat(factor, HEAD_DIM)[None, :]
    return (w_q.astype(F32) * col_factor).astype(BF16), (w_k.astype(F32) * col_factor).astype(BF16)


def solution(mesh):
    cp_size, dp_size = mesh.shape["cp"], mesh.shape["dp"]
    sizes = (dp_size // 8, 4)
    swap = []
    for quad in range(dp_size // 2):
        for x in range(cp_size):
            src_dp = 2 * quad + 1 - x // 2
            dst_x = cp_size - 1 - x
            dst_dp = 2 * quad + 1 - dst_x // 2
            swap.append((src_dp * cp_size + x, dst_dp * cp_size + dst_x))
            home = (2 * quad + x // 2) * cp_size + x
            swap.append((home, home))

    def device_body(hidden, pos_ids, w_q, w_k, w_v, w_o):
        inv_freq = ROPE_THETA ** (-np.arange(HEAD_DIM // 2) * (2.0 / HEAD_DIM))
        freq = jnp.asarray(np.concatenate([inv_freq, inv_freq])[None, :], F32)
        out, peak = attend(hidden[0], pos_ids.reshape(4, 128), freq, w_q, w_k, w_v, w_o)
        swapped = lax.ppermute(out, ("dp", "cp"), swap)
        head_max = global_peak(peak, sizes)[:, 0]
        w_q_new, w_k_new = clip_weights(head_max, w_q, w_k)
        return swapped[None], head_max, w_q_new, w_k_new

    return jax.shard_map(
        device_body,
        mesh=mesh,
        in_specs=(P("dp", "cp", None), P("cp"), P(None, None), P(None, None), P(None, None), P(None, None)),
        out_specs=(P("dp", "cp", None), P(None), P(None, None), P(None, None)),
        check_vma=False,
    )
```

```python
import functools

import jax
import jax.numpy as jnp
import numpy as np
from jax import lax
from jax.experimental import pallas as pl
from jax.experimental.pallas import tpu as pltpu
from jax.sharding import PartitionSpec as P

HEAD_DIM = 128
TAU_CLIP = 100.0
ROPE_THETA = 50000.0
SCALE = HEAD_DIM ** -0.5
LOG2E = 1.4426950408889634
MESH = pl.DeviceIdType.MESH

PIECE = 512
HALF = 256
MODEL = 2048
COLS = 1024
HEADS = 8
OWN, FAR, NEAR, LAST = 0, 1, 2, 3
TABLE_OF = (0, 1, 2, 0)
F32, BF16 = jnp.float32, jnp.bfloat16


def attend_kernel(hid, pos, freq, w_q, w_k, w_v, w_o, out, peak,
                  hbuf, wk, wv, w_pair, qbuf, kbuf, vbuf, acc, run_max, run_sum, cos_t, sin_t, pos_all,
                  bias, top_all, wsem, send, recv, psend, precv, osem, tsend, trecv):
    x = lax.axis_index("cp")
    d = lax.axis_index("dp")
    core = lax.rem(d, 2)
    home = core == x // 2
    away = core != x // 2
    partner = d + 1 - 2 * core
    pair = x + 1 - 2 * lax.rem(x, 2)
    far_x = 3 - x
    piece_of = (x, far_x, pair, 3 - pair)
    col0 = pl.multiple_of(core * COLS, COLS)

    def rows(kind, half):
        return pl.ds(pl.multiple_of(piece_of[kind] * PIECE + half * HALF, HALF), HALF)

    def remote(src, dst, s_sem, r_sem, dp, cp):
        return pltpu.make_async_remote_copy(src_ref=src, dst_ref=dst, send_sem=s_sem, recv_sem=r_sem,
                                            device_id={"dp": dp, "cp": cp}, device_id_type=MESH)

    w_copies = [pltpu.make_async_copy(src.at[:, pl.ds(col0, COLS)], dst, wsem.at[i])
                for i, (src, dst) in enumerate(((w_k, wk), (w_v, wv), (w_q, w_pair.at[0])))]
    w_copies.append(pltpu.make_async_copy(w_o.at[:, pl.ds(COLS, COLS)], w_pair.at[1], wsem.at[3]))
    wo_low = pltpu.make_async_copy(w_o.at[:, pl.ds(0, COLS)], w_pair.at[0], wsem.at[6])

    def half_rows(j):
        return pl.ds(pl.multiple_of(j * HALF, HALF), HALF)

    def own_local(j):
        return pltpu.make_async_copy(hid.at[half_rows(j), :], hbuf.at[rows(OWN, j), :], wsem.at[4 + j])

    @pl.when(home)
    def _():
        for j in range(2):
            own_local(j).start()
    for copy in w_copies:
        copy.start()

    barrier = pltpu.get_barrier_semaphore()
    for k in range(1, 4):
        pl.semaphore_signal(barrier, inc=1, device_id={"dp": d, "cp": lax.rem(x + k, 4)}, device_id_type=MESH)
    pl.semaphore_signal(barrier, inc=1, device_id={"dp": partner, "cp": x}, device_id_type=MESH)
    pl.semaphore_wait(barrier, 4)

    def own_copy(j, to_pair):
        src = hid.at[half_rows(j), :]
        dst = hbuf.at[rows(OWN, j), :]
        if to_pair:
            return remote(src, dst, send.at[j], recv.at[NEAR * 2 + j], d, pair)
        return remote(src, dst, send.at[2 + j], recv.at[OWN * 2 + j], partner, x)

    def away_copy(j):
        return remote(hid.at[half_rows(j), :], hbuf.at[rows(OWN, j), :], send.at[12 + j], recv.at[FAR * 2 + j], d, far_x)

    def far_to_pair(j):
        return remote(hbuf.at[rows(FAR, j), :], hbuf.at[rows(FAR, j), :], send.at[4 + j], recv.at[LAST * 2 + j], d, pair)

    def to_partner(kind, j):
        return remote(hbuf.at[rows(kind, j), :], hbuf.at[rows(kind, j), :], send.at[4 + 2 * kind + j], recv.at[kind * 2 + j], partner, x)

    pos_copies = [remote(pos, pos_all.at[x], psend.at[k - 1], precv.at[k - 1], d, lax.rem(x + k, 4)) for k in range(1, 4)]
    for copy in pos_copies:
        copy.start()

    @pl.when(home)
    def _():
        @pl.when(x != 3)
        def _():
            for j in range(2):
                own_copy(j, True).start()
        for j in range(2):
            own_copy(j, False).start()

    @pl.when(away)
    def _():
        for j in range(2):
            away_copy(j).start()

    def tables(kind):
        piece = piece_of[kind]
        row_i = lax.broadcasted_iota(jnp.int32, (64, 128), 0)
        col_i = lax.broadcasted_iota(jnp.int32, (64, 128), 1)
        low = col_i < 64

        def one(b):
            if kind == OWN:
                line = pos[pl.ds(b, 1), :]
            else:
                line = pos_all[pl.ds(piece, 1), pl.ds(b, 1), :].reshape(1, 128)
            line = jnp.broadcast_to(line.astype(F32), (64, 128))
            first = jnp.sum(jnp.where(row_i == col_i, line, 0.0), axis=1, keepdims=True)
            second = jnp.sum(jnp.where(row_i + 64 == col_i, line, 0.0), axis=1, keepdims=True)
            angle = jnp.where(low, first, second) * freq[...]
            cos_a, sin_a = jnp.cos(angle), jnp.sin(angle)
            cos_r, sin_r = pltpu.roll(cos_a, 64, 1), pltpu.roll(sin_a, 64, 1)
            at = pl.multiple_of(TABLE_OF[kind] * PIECE + b * 128, 128)
            cos_t[pl.ds(at, 64), :] = jnp.where(low, cos_a, cos_r)
            cos_t[pl.ds(at + 64, 64), :] = jnp.where(low, cos_r, cos_a)
            sin_t[pl.ds(at, 64), :] = jnp.where(low, -sin_a, sin_r)
            sin_t[pl.ds(at + 64, 64), :] = jnp.where(low, -sin_r, sin_a)

        def block(b, carry):
            one(2 * b)
            one(2 * b + 1)
            return carry

        lax.fori_loop(0, 2, block, 0)

    def rotate(t, cos_v, sin_v):
        parts = []
        for h in range(HEADS):
            u = t[:, h * HEAD_DIM:(h + 1) * HEAD_DIM]
            parts.append((u * cos_v + pltpu.roll(u, 64, 1) * sin_v).astype(BF16))
        return jnp.concatenate(parts, axis=1)

    def project(kind, half, with_q):
        at = rows(kind, half)
        table = pl.ds(pl.multiple_of(TABLE_OF[kind] * PIECE + half * HALF, HALF), HALF)
        cos_v, sin_v = cos_t[table, :], sin_t[table, :]
        h = hbuf[at, :]
        kbuf[at, :] = rotate(jnp.dot(h, wk[...], preferred_element_type=F32), cos_v, sin_v)
        vbuf[at, :] = jnp.dot(h, wv[...], preferred_element_type=F32).astype(BF16)
        if with_q:
            q_at = pl.ds(pl.multiple_of(half * HALF, HALF), HALF)
            qbuf[kind, q_at, :] = rotate(jnp.dot(h, w_pair[0], preferred_element_type=F32), cos_v, sin_v)

    def tile(slot, piece, diagonal):
        key0 = pl.multiple_of(piece * PIECE, PIECE)
        units = [(h, qb) for h in range(HEADS) for qb in range(2)]

        def scores(h, qb):
            n_keys = HALF * (qb + 1) if diagonal else PIECE
            cols = pl.ds(h * HEAD_DIM, HEAD_DIM)
            s = lax.dot_general(qbuf[slot, pl.ds(qb * HALF, HALF), cols], kbuf[pl.ds(key0, n_keys), cols],
                                (((1,), (1,)), ((), ())), preferred_element_type=F32)
            if diagonal:
                last = s[:, n_keys - HALF:] + bias[...]
                s = last if qb == 0 else jnp.concatenate([s[:, :n_keys - HALF], last], axis=1)
            return s

        results = []
        s = scores(*units[0])
        for i, (h, qb) in enumerate(units):
            s_next = scores(*units[i + 1]) if i + 1 < len(units) else None
            at = pl.ds(qb * HALF, HALF)
            n_keys = s.shape[1]
            top = jnp.max(s, axis=1, keepdims=True)
            old = None if diagonal else run_max[slot, h, at, :]
            new = jnp.broadcast_to(top, (HALF, 128)) if diagonal else jnp.maximum(old, top)
            p = jnp.exp2((s - jnp.concatenate([new] * (n_keys // 128), axis=1)) * (SCALE * LOG2E))
            total = p[:, :128]
            for g in range(1, n_keys // 128):
                total = total + p[:, g * 128:(g + 1) * 128]
            part = jnp.dot(p.astype(BF16), vbuf[pl.ds(key0, n_keys), pl.ds(h * HEAD_DIM, HEAD_DIM)],
                           preferred_element_type=F32)
            results.append((old, new, total, part))
            s = s_next
        for (h, qb), (old, new, total, part) in zip(units, results):
            at, cols = pl.ds(qb * HALF, HALF), pl.ds(h * HEAD_DIM, HEAD_DIM)
            if not diagonal:
                fade = jnp.exp2((old - new) * (SCALE * LOG2E))
                total = total + run_sum[slot, h, at, :] * fade
                part = part + acc[slot, at, cols] * fade
            run_max[slot, h, at, :] = new
            run_sum[slot, h, at, :] = total
            acc[slot, at, cols] = part

    def arrive(kind, j):
        @pl.when(home)
        def _():
            if kind == OWN:
                own_local(j).wait()
            else:
                away_copy(j).wait_recv() if kind == FAR else own_copy(j, True).wait_recv() if kind == NEAR else far_to_pair(j).wait_recv()
                if kind == FAR:
                    @pl.when(x != 0)
                    def _():
                        far_to_pair(j).start()
                to_partner(kind, j).start()

        @pl.when(away)
        def _():
            if kind == OWN:
                own_copy(j, False).wait_recv()
            else:
                to_partner(kind, j).wait_recv()

    bias[...] = jnp.where(lax.broadcasted_iota(jnp.int32, (HALF, HALF), 0) >= lax.broadcasted_iota(jnp.int32, (HALF, HALF), 1),
                          0.0, -jnp.inf)
    tables(OWN)
    for copy in pos_copies:
        copy.wait_recv()
    tables(FAR)
    tables(NEAR)
    for i in range(3):
        w_copies[i].wait()

    def own_half(j, carry):
        arrive(OWN, j)
        project(OWN, j, True)
        return carry

    lax.fori_loop(0, 2, own_half, 0)

    def far_half(j, carry):
        arrive(FAR, j)

        @pl.when(x != 2)
        def _():
            arrive(NEAR, j)

        project(FAR, j, True)

        @pl.when(x != 2)
        def _():
            project(NEAR, j, False)
        return carry

    lax.fori_loop(0, 2, far_half, 0)
    wo_low.start()
    tables(LAST)

    def diagonal_tile(slot, carry):
        tile(slot, jnp.where(slot == OWN, x, far_x), True)
        return carry

    lax.fori_loop(0, 2, diagonal_tile, 0)

    later = jnp.where(x < 2, FAR, OWN)

    def near_tile(i, carry):
        slot = jnp.where(i == 0, later, i - 1)
        piece = jnp.where(i == 0, jnp.minimum(x, far_x), pair)

        @pl.when((i == 0) | ((i == 1) & (lax.rem(x, 2) == 1)) | ((i == 2) & (x < 2)))
        def _():
            tile(slot, piece, False)
        return carry

    lax.fori_loop(0, 3, near_tile, 0)

    early = 1 - later
    mine = jnp.where(core == 0, early, later)
    exchange = remote(qbuf.at[1 - mine], qbuf.at[2], osem.at[0], osem.at[1], partner, x)
    own_rows = pl.ds(pl.multiple_of(x * PIECE, PIECE), PIECE)

    def out_copy(part):
        cols = pl.ds(pl.multiple_of(part * COLS, COLS), COLS)
        return pltpu.make_async_copy(hbuf.at[own_rows, cols], out.at[:, cols], wsem.at[7 + part])

    def finish(slot):
        for h in range(HEADS):
            cols = pl.ds(h * HEAD_DIM, HEAD_DIM)
            total = jnp.sum(run_sum[slot, h, :, :], axis=1, keepdims=True)
            qbuf[slot, :, cols] = (acc[slot, :, cols] / total).astype(BF16)

    def output(part):
        heads = jnp.concatenate([qbuf[jnp.where(core == 0, mine, 2)], qbuf[jnp.where(core == 0, 2, mine)]], axis=1)
        value = jnp.dot(heads, w_pair[part], preferred_element_type=F32)
        hbuf[own_rows, pl.ds(pl.multiple_of(part * COLS, COLS), COLS)] = value.astype(BF16)
        out_copy(part).start()

    w_copies[3].wait()
    wo_low.wait()
    outer = (x == 0) | (x == 3)

    @pl.when(outer)
    def _():
        finish(early)

        @pl.when(core == 1)
        def _():
            exchange.start()

        @pl.when(core == 0)
        def _():
            exchange.wait_recv()

            def one(part, carry):
                output(part)
                return carry

            lax.fori_loop(0, 2, one, 0)

    @pl.when(x != 1)
    def _():
        def last_half(j, carry):
            arrive(LAST, j)
            project(LAST, j, False)
            return carry
        lax.fori_loop(0, 2, last_half, 0)

    def last_tile(slot, carry):
        @pl.when(((slot == OWN) & (x >= 2)) | ((slot == FAR) & (lax.rem(x, 2) == 0)))
        def _():
            tile(slot, 3 - pair, False)
        return carry

    lax.fori_loop(0, 2, last_tile, 0)

    finish(later)

    @pl.when(core == 0)
    def _():
        exchange.start()

    top_all[0] = jnp.full((2 * HEADS, 128), -jnp.inf, F32)
    for h in range(HEADS):
        top = jnp.maximum(jnp.max(run_max[0, h, :, :], axis=0, keepdims=True), jnp.max(run_max[1, h, :, :], axis=0, keepdims=True))
        top_all[0, pl.ds(core * HEADS + h, 1), :] = top * SCALE
    top_copies = [remote(top_all.at[0], top_all.at[k], tsend.at[k - 1], trecv.at[k - 1], d, lax.rem(x + k, 4)) for k in range(1, 4)]
    top_copies.append(remote(top_all.at[4], top_all.at[5], tsend.at[3], trecv.at[3], partner, x))
    for copy in top_copies[:3]:
        copy.start()

    @pl.when(jnp.logical_not(outer))
    def _():
        finish(early)

        @pl.when(core == 1)
        def _():
            exchange.start()

    busy = (core == 1) | jnp.logical_not(outer)

    @pl.when(busy)
    def _():
        exchange.wait_recv()
        output(0)

    best = top_all[0]
    for k in range(3):
        top_copies[k].wait_recv()
        best = jnp.maximum(best, top_all[k + 1])
    top_all[4] = best
    top_copies[3].start()

    @pl.when(busy)
    def _():
        output(1)

    top_copies[3].wait_recv()
    peak[...] = jnp.maximum(top_all[4], top_all[5])
    for copy in top_copies:
        copy.wait_send()
    for part in range(2):
        out_copy(part).wait()

    exchange.wait_send()
    for copy in pos_copies:
        copy.wait_send()

    @pl.when(away)
    def _():
        for j in range(2):
            away_copy(j).wait_send()

    @pl.when(home)
    def _():
        for j in range(2):
            own_copy(j, False).wait_send()
            to_partner(FAR, j).wait_send()

        @pl.when(x != 3)
        def _():
            for j in range(2):
                own_copy(j, True).wait_send()

        @pl.when(x != 0)
        def _():
            for j in range(2):
                far_to_pair(j).wait_send()

        @pl.when(x != 2)
        def _():
            for j in range(2):
                to_partner(NEAR, j).wait_send()

        @pl.when(x != 1)
        def _():
            for j in range(2):
                to_partner(LAST, j).wait_send()


def attend(hid, pos, freq, w_q, w_k, w_v, w_o):
    any_spec = pl.BlockSpec(memory_space=pl.ANY)
    vmem = pl.BlockSpec(memory_space=pltpu.VMEM)
    return pl.pallas_call(
        attend_kernel,
        name="attend",
        out_shape=[jax.ShapeDtypeStruct((PIECE, MODEL), BF16), jax.ShapeDtypeStruct((2 * HEADS, 128), F32)],
        in_specs=[any_spec, vmem, vmem, any_spec, any_spec, any_spec, any_spec],
        out_specs=[any_spec, vmem],
        scratch_shapes=[
            pltpu.VMEM((4 * PIECE, MODEL), BF16),
            pltpu.VMEM((MODEL, COLS), BF16), pltpu.VMEM((MODEL, COLS), BF16), pltpu.VMEM((2, MODEL, COLS), BF16),
            pltpu.VMEM((3, PIECE, COLS), BF16), pltpu.VMEM((4 * PIECE, COLS), BF16), pltpu.VMEM((4 * PIECE, COLS), BF16),
            pltpu.VMEM((2, PIECE, COLS), F32), pltpu.VMEM((2, HEADS, PIECE, 128), F32), pltpu.VMEM((2, HEADS, PIECE, 128), F32),
            pltpu.VMEM((3 * PIECE, 128), F32), pltpu.VMEM((3 * PIECE, 128), F32), pltpu.VMEM((4, 4, 128), jnp.int32),
            pltpu.VMEM((HALF, HALF), F32), pltpu.VMEM((6, 2 * HEADS, 128), F32),
            pltpu.SemaphoreType.DMA((9,)), pltpu.SemaphoreType.DMA((14,)), pltpu.SemaphoreType.DMA((8,)),
            pltpu.SemaphoreType.DMA((3,)), pltpu.SemaphoreType.DMA((3,)), pltpu.SemaphoreType.DMA((2,)),
            pltpu.SemaphoreType.DMA((4,)), pltpu.SemaphoreType.DMA((4,)),
        ],
        compiler_params=pltpu.CompilerParams(collective_id=0, has_side_effects=True, vmem_limit_bytes=67043328),
        cost_estimate=pl.CostEstimate(flops=31_000_000_000, bytes_accessed=26_000_000, transcendentals=11_000_000),
    )(hid, pos, freq, w_q, w_k, w_v, w_o)


def peak_kernel(sizes, peak, best, cur, slots, send, recv):
    n_z, n_y = sizes
    x = lax.axis_index("cp")
    d = lax.axis_index("dp")
    core, y, z = lax.rem(d, 2), lax.rem(d // 2, n_y), d // (2 * n_y)
    rounds = [
        [((z * n_y + lax.rem(y + k, n_y)) * 2 + core, x) for k in range(1, n_y)],
        [((lax.rem(z + k, n_z) * n_y + y) * 2 + core, x) for k in range(1, n_z)],
    ]
    barrier = pltpu.get_barrier_semaphore()
    total = 0
    for peers in rounds:
        for dp, cp in peers:
            pl.semaphore_signal(barrier, inc=1, device_id={"dp": dp, "cp": cp}, device_id_type=MESH)
            total += 1
    cur[0] = peak[...]
    pl.semaphore_wait(barrier, total)
    index = 0
    copies = []
    for r, peers in enumerate(rounds):
        batch = []
        for dp, cp in peers:
            batch.append((index, pltpu.make_async_remote_copy(
                src_ref=cur.at[r], dst_ref=slots.at[index], send_sem=send.at[index], recv_sem=recv.at[index],
                device_id={"dp": dp, "cp": cp}, device_id_type=MESH)))
            index += 1
        for _, copy in batch:
            copy.start()
        value = cur[r]
        for i, copy in batch:
            copy.wait_recv()
            value = jnp.maximum(value, slots[i])
        if r + 1 < len(rounds):
            cur[r + 1] = value
        else:
            best[...] = value
        copies += batch
    for _, copy in copies:
        copy.wait_send()


def global_peak(peak, sizes):
    n_copies = sum(n - 1 for n in sizes)
    vmem = pl.BlockSpec(memory_space=pltpu.VMEM)
    shape = peak.shape
    return pl.pallas_call(
        functools.partial(peak_kernel, sizes),
        name="global_peak",
        out_shape=jax.ShapeDtypeStruct(shape, F32),
        in_specs=[vmem], out_specs=vmem,
        scratch_shapes=[pltpu.VMEM((2,) + shape, F32), pltpu.VMEM((n_copies,) + shape, F32),
                        pltpu.SemaphoreType.DMA((n_copies,)), pltpu.SemaphoreType.DMA((n_copies,))],
        compiler_params=pltpu.CompilerParams(collective_id=1, has_side_effects=True),
        cost_estimate=pl.CostEstimate(flops=10_000_000, bytes_accessed=8192, transcendentals=0),
    )(peak)


def clip_weights(head_max, w_q, w_k):
    factor = jnp.where(head_max > TAU_CLIP, jnp.sqrt(TAU_CLIP / head_max), 1.0)
    col_factor = jnp.repeat(factor, HEAD_DIM)[None, :]
    return (w_q.astype(F32) * col_factor).astype(BF16), (w_k.astype(F32) * col_factor).astype(BF16)


def solution(mesh):
    cp_size, dp_size = mesh.shape["cp"], mesh.shape["dp"]
    sizes = (dp_size // 8, 4)
    swap = []
    for quad in range(dp_size // 2):
        for x in range(cp_size):
            src_dp = 2 * quad + 1 - x // 2
            dst_x = cp_size - 1 - x
            dst_dp = 2 * quad + 1 - dst_x // 2
            swap.append((src_dp * cp_size + x, dst_dp * cp_size + dst_x))
            home = (2 * quad + x // 2) * cp_size + x
            swap.append((home, home))

    def device_body(hidden, pos_ids, w_q, w_k, w_v, w_o):
        inv_freq = ROPE_THETA ** (-np.arange(HEAD_DIM // 2) * (2.0 / HEAD_DIM))
        freq = jnp.asarray(np.concatenate([inv_freq, inv_freq])[None, :], F32)
        out, peak = attend(hidden[0], pos_ids.reshape(4, 128), freq, w_q, w_k, w_v, w_o)
        swapped = lax.ppermute(out, ("dp", "cp"), swap)
        head_max = global_peak(peak, sizes)[:, 0]
        w_q_new, w_k_new = clip_weights(head_max, w_q, w_k)
        return swapped[None], head_max, w_q_new, w_k_new

    return jax.shard_map(
        device_body,
        mesh=mesh,
        in_specs=(P("dp", "cp", None), P("cp"), P(None, None), P(None, None), P(None, None), P(None, None)),
        out_specs=(P("dp", "cp", None), P(None), P(None, None), P(None, None)),
        check_vma=False,
    )
```

```python
import functools

import jax
import jax.numpy as jnp
import numpy as np
from jax import lax
from jax.experimental import pallas as pl
from jax.experimental.pallas import tpu as pltpu
from jax.sharding import PartitionSpec as P

HEAD_DIM = 128
TAU_CLIP = 100.0
ROPE_THETA = 50000.0
SCALE = HEAD_DIM ** -0.5
LOG2E = 1.4426950408889634
MESH = pl.DeviceIdType.MESH

PIECE = 512
HALF = 256
MODEL = 2048
COLS = 1024
HEADS = 8
OWN, FAR, NEAR, LAST = 0, 1, 2, 3
TABLE_OF = (0, 1, 2, 0)
F32, BF16 = jnp.float32, jnp.bfloat16


def attend_kernel(hid, pos, freq, w_q, w_k, w_v, w_o, out, peak,
                  hbuf, wk, wv, w_pair, qbuf, kbuf, vbuf, acc, run_max, run_sum, cos_t, sin_t, pos_all,
                  bias, top_all, wsem, send, recv, psend, precv, osem, tsend, trecv):
    x = lax.axis_index("cp")
    d = lax.axis_index("dp")
    core = lax.rem(d, 2)
    home = core == x // 2
    away = core != x // 2
    partner = d + 1 - 2 * core
    pair = x + 1 - 2 * lax.rem(x, 2)
    far_x = 3 - x
    piece_of = (x, far_x, pair, 3 - pair)
    col0 = pl.multiple_of(core * COLS, COLS)

    def rows(kind, half):
        return pl.ds(pl.multiple_of(piece_of[kind] * PIECE + half * HALF, HALF), HALF)

    def remote(src, dst, s_sem, r_sem, dp, cp):
        return pltpu.make_async_remote_copy(src_ref=src, dst_ref=dst, send_sem=s_sem, recv_sem=r_sem,
                                            device_id={"dp": dp, "cp": cp}, device_id_type=MESH)

    w_copies = [pltpu.make_async_copy(src.at[:, pl.ds(col0, COLS)], dst, wsem.at[i])
                for i, (src, dst) in enumerate(((w_k, wk), (w_v, wv), (w_q, w_pair.at[0])))]
    w_copies.append(pltpu.make_async_copy(w_o.at[:, pl.ds(COLS, COLS)], w_pair.at[1], wsem.at[3]))
    wo_low = pltpu.make_async_copy(w_o.at[:, pl.ds(0, COLS)], w_pair.at[0], wsem.at[6])

    def half_rows(j):
        return pl.ds(pl.multiple_of(j * HALF, HALF), HALF)

    def own_local(j):
        return pltpu.make_async_copy(hid.at[half_rows(j), :], hbuf.at[rows(OWN, j), :], wsem.at[4 + j])

    @pl.when(home)
    def _():
        for j in range(2):
            own_local(j).start()
    for copy in w_copies:
        copy.start()

    barrier = pltpu.get_barrier_semaphore()
    for k in range(1, 4):
        pl.semaphore_signal(barrier, inc=1, device_id={"dp": d, "cp": lax.rem(x + k, 4)}, device_id_type=MESH)
    pl.semaphore_signal(barrier, inc=1, device_id={"dp": partner, "cp": x}, device_id_type=MESH)
    pl.semaphore_wait(barrier, 4)

    def own_copy(j, to_pair):
        src = hid.at[half_rows(j), :]
        dst = hbuf.at[rows(OWN, j), :]
        if to_pair:
            return remote(src, dst, send.at[j], recv.at[NEAR * 2 + j], d, pair)
        return remote(src, dst, send.at[2 + j], recv.at[OWN * 2 + j], partner, x)

    def away_copy(j):
        return remote(hid.at[half_rows(j), :], hbuf.at[rows(OWN, j), :], send.at[12 + j], recv.at[FAR * 2 + j], d, far_x)

    def far_to_pair(j):
        return remote(hbuf.at[rows(FAR, j), :], hbuf.at[rows(FAR, j), :], send.at[4 + j], recv.at[LAST * 2 + j], d, pair)

    def to_partner(kind, j):
        return remote(hbuf.at[rows(kind, j), :], hbuf.at[rows(kind, j), :], send.at[4 + 2 * kind + j], recv.at[kind * 2 + j], partner, x)

    pos_copies = [remote(pos, pos_all.at[x], psend.at[k - 1], precv.at[k - 1], d, lax.rem(x + k, 4)) for k in range(1, 4)]
    for copy in pos_copies:
        copy.start()

    @pl.when(home)
    def _():
        @pl.when(x != 3)
        def _():
            for j in range(2):
                own_copy(j, True).start()
        for j in range(2):
            own_copy(j, False).start()

    @pl.when(away)
    def _():
        for j in range(2):
            away_copy(j).start()

    def tables(kind):
        piece = piece_of[kind]
        row_i = lax.broadcasted_iota(jnp.int32, (64, 128), 0)
        col_i = lax.broadcasted_iota(jnp.int32, (64, 128), 1)
        low = col_i < 64

        def one(b):
            if kind == OWN:
                line = pos[pl.ds(b, 1), :]
            else:
                line = pos_all[pl.ds(piece, 1), pl.ds(b, 1), :].reshape(1, 128)
            line = jnp.broadcast_to(line.astype(F32), (64, 128))
            first = jnp.sum(jnp.where(row_i == col_i, line, 0.0), axis=1, keepdims=True)
            second = jnp.sum(jnp.where(row_i + 64 == col_i, line, 0.0), axis=1, keepdims=True)
            angle = jnp.where(low, first, second) * freq[...]
            cos_a, sin_a = jnp.cos(angle), jnp.sin(angle)
            cos_r, sin_r = pltpu.roll(cos_a, 64, 1), pltpu.roll(sin_a, 64, 1)
            at = pl.multiple_of(TABLE_OF[kind] * PIECE + b * 128, 128)
            cos_t[pl.ds(at, 64), :] = jnp.where(low, cos_a, cos_r)
            cos_t[pl.ds(at + 64, 64), :] = jnp.where(low, cos_r, cos_a)
            sin_t[pl.ds(at, 64), :] = jnp.where(low, -sin_a, sin_r)
            sin_t[pl.ds(at + 64, 64), :] = jnp.where(low, -sin_r, sin_a)

        def block(b, carry):
            one(2 * b)
            one(2 * b + 1)
            return carry

        lax.fori_loop(0, 2, block, 0)

    def rotate(t, cos_v, sin_v):
        parts = []
        for h in range(HEADS):
            u = t[:, h * HEAD_DIM:(h + 1) * HEAD_DIM]
            parts.append((u * cos_v + pltpu.roll(u, 64, 1) * sin_v).astype(BF16))
        return jnp.concatenate(parts, axis=1)

    def project(kind, half, with_q):
        at = rows(kind, half)
        table = pl.ds(pl.multiple_of(TABLE_OF[kind] * PIECE + half * HALF, HALF), HALF)
        cos_v, sin_v = cos_t[table, :], sin_t[table, :]
        h = hbuf[at, :]
        kbuf[at, :] = rotate(jnp.dot(h, wk[...], preferred_element_type=F32), cos_v, sin_v)
        vbuf[at, :] = jnp.dot(h, wv[...], preferred_element_type=F32).astype(BF16)
        if with_q:
            q_at = pl.ds(pl.multiple_of(half * HALF, HALF), HALF)
            qbuf[kind, q_at, :] = rotate(jnp.dot(h, w_pair[0], preferred_element_type=F32), cos_v, sin_v)

    def tile(slot, piece, diagonal):
        key0 = pl.multiple_of(piece * PIECE, PIECE)
        units = [(h, qb) for h in range(HEADS) for qb in range(2)]

        def scores(h, qb):
            n_keys = HALF * (qb + 1) if diagonal else PIECE
            cols = pl.ds(h * HEAD_DIM, HEAD_DIM)
            s = lax.dot_general(qbuf[slot, pl.ds(qb * HALF, HALF), cols], kbuf[pl.ds(key0, n_keys), cols],
                                (((1,), (1,)), ((), ())), preferred_element_type=F32)
            if diagonal:
                last = s[:, n_keys - HALF:] + bias[...]
                s = last if qb == 0 else jnp.concatenate([s[:, :n_keys - HALF], last], axis=1)
            return s

        results = []
        s = scores(*units[0])
        for i, (h, qb) in enumerate(units):
            s_next = scores(*units[i + 1]) if i + 1 < len(units) else None
            at = pl.ds(qb * HALF, HALF)
            n_keys = s.shape[1]
            top = jnp.max(s, axis=1, keepdims=True)
            old = None if diagonal else run_max[slot, h, at, :]
            new = jnp.broadcast_to(top, (HALF, 128)) if diagonal else jnp.maximum(old, top)
            p = jnp.exp2((s - jnp.concatenate([new] * (n_keys // 128), axis=1)) * (SCALE * LOG2E))
            total = p[:, :128]
            for g in range(1, n_keys // 128):
                total = total + p[:, g * 128:(g + 1) * 128]
            part = jnp.dot(p.astype(BF16), vbuf[pl.ds(key0, n_keys), pl.ds(h * HEAD_DIM, HEAD_DIM)],
                           preferred_element_type=F32)
            results.append((old, new, total, part))
            s = s_next
        for (h, qb), (old, new, total, part) in zip(units, results):
            at, cols = pl.ds(qb * HALF, HALF), pl.ds(h * HEAD_DIM, HEAD_DIM)
            if not diagonal:
                fade = jnp.exp2((old - new) * (SCALE * LOG2E))
                total = total + run_sum[slot, h, at, :] * fade
                part = part + acc[slot, at, cols] * fade
            run_max[slot, h, at, :] = new
            run_sum[slot, h, at, :] = total
            acc[slot, at, cols] = part

    def arrive(kind, j):
        @pl.when(home)
        def _():
            if kind == OWN:
                own_local(j).wait()
            else:
                away_copy(j).wait_recv() if kind == FAR else own_copy(j, True).wait_recv() if kind == NEAR else far_to_pair(j).wait_recv()
                if kind == FAR:
                    @pl.when(x != 0)
                    def _():
                        far_to_pair(j).start()
                to_partner(kind, j).start()

        @pl.when(away)
        def _():
            if kind == OWN:
                own_copy(j, False).wait_recv()
            else:
                to_partner(kind, j).wait_recv()

    bias[...] = jnp.where(lax.broadcasted_iota(jnp.int32, (HALF, HALF), 0) >= lax.broadcasted_iota(jnp.int32, (HALF, HALF), 1),
                          0.0, -jnp.inf)
    tables(OWN)
    for copy in pos_copies:
        copy.wait_recv()
    tables(FAR)
    tables(NEAR)
    for i in range(3):
        w_copies[i].wait()

    def own_half(j, carry):
        arrive(OWN, j)
        project(OWN, j, True)
        return carry

    lax.fori_loop(0, 2, own_half, 0)
    @pl.when(x >= 0)
    def _():
        tile(OWN, x, True)


    def far_half(j, carry):
        arrive(FAR, j)

        @pl.when(x != 2)
        def _():
            arrive(NEAR, j)

        project(FAR, j, True)

        @pl.when(x != 2)
        def _():
            project(NEAR, j, False)
        return carry

    lax.fori_loop(0, 2, far_half, 0)
    wo_low.start()
    tables(LAST)

    @pl.when(x >= 0)
    def _():
        tile(FAR, far_x, True)

    later = jnp.where(x < 2, FAR, OWN)

    def near_tile(i, carry):
        slot = jnp.where(i == 0, later, i - 1)
        piece = jnp.where(i == 0, jnp.minimum(x, far_x), pair)

        @pl.when((i == 0) | ((i == 1) & (lax.rem(x, 2) == 1)) | ((i == 2) & (x < 2)))
        def _():
            tile(slot, piece, False)
        return carry

    lax.fori_loop(0, 3, near_tile, 0)

    early = 1 - later
    mine = jnp.where(core == 0, early, later)
    exchange = remote(qbuf.at[1 - mine], qbuf.at[2], osem.at[0], osem.at[1], partner, x)
    own_rows = pl.ds(pl.multiple_of(x * PIECE, PIECE), PIECE)

    def out_copy(part):
        cols = pl.ds(pl.multiple_of(part * COLS, COLS), COLS)
        return pltpu.make_async_copy(hbuf.at[own_rows, cols], out.at[:, cols], wsem.at[7 + part])

    def finish(slot):
        for h in range(HEADS):
            cols = pl.ds(h * HEAD_DIM, HEAD_DIM)
            total = jnp.sum(run_sum[slot, h, :, :], axis=1, keepdims=True)
            qbuf[slot, :, cols] = (acc[slot, :, cols] / total).astype(BF16)

    def output(part):
        heads = jnp.concatenate([qbuf[jnp.where(core == 0, mine, 2)], qbuf[jnp.where(core == 0, 2, mine)]], axis=1)
        value = jnp.dot(heads, w_pair[part], preferred_element_type=F32)
        hbuf[own_rows, pl.ds(pl.multiple_of(part * COLS, COLS), COLS)] = value.astype(BF16)
        out_copy(part).start()

    outer = (x == 0) | (x == 3)

    @pl.when(outer)
    def _():
        finish(early)

        @pl.when(core == 1)
        def _():
            exchange.start()

    @pl.when(x != 1)
    def _():
        def last_half(j, carry):
            arrive(LAST, j)
            project(LAST, j, False)
            return carry
        lax.fori_loop(0, 2, last_half, 0)

    def last_tile(slot, carry):
        @pl.when(((slot == OWN) & (x >= 2)) | ((slot == FAR) & (lax.rem(x, 2) == 0)))
        def _():
            tile(slot, 3 - pair, False)
        return carry

    lax.fori_loop(0, 2, last_tile, 0)

    finish(later)

    @pl.when(core == 0)
    def _():
        exchange.start()

    top_all[0] = jnp.full((2 * HEADS, 128), -jnp.inf, F32)
    for h in range(HEADS):
        top = jnp.maximum(jnp.max(run_max[0, h, :, :], axis=0, keepdims=True), jnp.max(run_max[1, h, :, :], axis=0, keepdims=True))
        top_all[0, pl.ds(core * HEADS + h, 1), :] = top * SCALE
    top_copies = [remote(top_all.at[0], top_all.at[k], tsend.at[k - 1], trecv.at[k - 1], d, lax.rem(x + k, 4)) for k in range(1, 4)]
    top_copies.append(remote(top_all.at[4], top_all.at[5], tsend.at[3], trecv.at[3], partner, x))
    for copy in top_copies[:3]:
        copy.start()

    @pl.when(jnp.logical_not(outer))
    def _():
        finish(early)

        @pl.when(core == 1)
        def _():
            exchange.start()

    w_copies[3].wait()
    wo_low.wait()
    exchange.wait_recv()

    @pl.when(x >= 0)
    def _():
        output(0)

    best = top_all[0]
    for k in range(3):
        top_copies[k].wait_recv()
        best = jnp.maximum(best, top_all[k + 1])
    top_all[4] = best
    top_copies[3].start()

    @pl.when(x >= 0)
    def _():
        output(1)

    top_copies[3].wait_recv()
    peak[...] = jnp.maximum(top_all[4], top_all[5])
    for copy in top_copies:
        copy.wait_send()
    for part in range(2):
        out_copy(part).wait()

    exchange.wait_send()
    for copy in pos_copies:
        copy.wait_send()

    @pl.when(away)
    def _():
        for j in range(2):
            away_copy(j).wait_send()

    @pl.when(home)
    def _():
        for j in range(2):
            own_copy(j, False).wait_send()
            to_partner(FAR, j).wait_send()

        @pl.when(x != 3)
        def _():
            for j in range(2):
                own_copy(j, True).wait_send()

        @pl.when(x != 0)
        def _():
            for j in range(2):
                far_to_pair(j).wait_send()

        @pl.when(x != 2)
        def _():
            for j in range(2):
                to_partner(NEAR, j).wait_send()

        @pl.when(x != 1)
        def _():
            for j in range(2):
                to_partner(LAST, j).wait_send()


def attend(hid, pos, freq, w_q, w_k, w_v, w_o):
    any_spec = pl.BlockSpec(memory_space=pl.ANY)
    vmem = pl.BlockSpec(memory_space=pltpu.VMEM)
    return pl.pallas_call(
        attend_kernel,
        name="attend",
        out_shape=[jax.ShapeDtypeStruct((PIECE, MODEL), BF16), jax.ShapeDtypeStruct((2 * HEADS, 128), F32)],
        in_specs=[any_spec, vmem, vmem, any_spec, any_spec, any_spec, any_spec],
        out_specs=[any_spec, vmem],
        scratch_shapes=[
            pltpu.VMEM((4 * PIECE, MODEL), BF16),
            pltpu.VMEM((MODEL, COLS), BF16), pltpu.VMEM((MODEL, COLS), BF16), pltpu.VMEM((2, MODEL, COLS), BF16),
            pltpu.VMEM((3, PIECE, COLS), BF16), pltpu.VMEM((4 * PIECE, COLS), BF16), pltpu.VMEM((4 * PIECE, COLS), BF16),
            pltpu.VMEM((2, PIECE, COLS), F32), pltpu.VMEM((2, HEADS, PIECE, 128), F32), pltpu.VMEM((2, HEADS, PIECE, 128), F32),
            pltpu.VMEM((3 * PIECE, 128), F32), pltpu.VMEM((3 * PIECE, 128), F32), pltpu.VMEM((4, 4, 128), jnp.int32),
            pltpu.VMEM((HALF, HALF), F32), pltpu.VMEM((6, 2 * HEADS, 128), F32),
            pltpu.SemaphoreType.DMA((9,)), pltpu.SemaphoreType.DMA((14,)), pltpu.SemaphoreType.DMA((8,)),
            pltpu.SemaphoreType.DMA((3,)), pltpu.SemaphoreType.DMA((3,)), pltpu.SemaphoreType.DMA((2,)),
            pltpu.SemaphoreType.DMA((4,)), pltpu.SemaphoreType.DMA((4,)),
        ],
        compiler_params=pltpu.CompilerParams(collective_id=0, has_side_effects=True, vmem_limit_bytes=67043328),
        cost_estimate=pl.CostEstimate(flops=31_000_000_000, bytes_accessed=26_000_000, transcendentals=11_000_000),
    )(hid, pos, freq, w_q, w_k, w_v, w_o)


def peak_kernel(sizes, peak, best, cur, slots, send, recv):
    n_z, n_y = sizes
    x = lax.axis_index("cp")
    d = lax.axis_index("dp")
    core, y, z = lax.rem(d, 2), lax.rem(d // 2, n_y), d // (2 * n_y)
    rounds = [
        [((z * n_y + lax.rem(y + k, n_y)) * 2 + core, x) for k in range(1, n_y)],
        [((lax.rem(z + k, n_z) * n_y + y) * 2 + core, x) for k in range(1, n_z)],
    ]
    barrier = pltpu.get_barrier_semaphore()
    total = 0
    for peers in rounds:
        for dp, cp in peers:
            pl.semaphore_signal(barrier, inc=1, device_id={"dp": dp, "cp": cp}, device_id_type=MESH)
            total += 1
    cur[0] = peak[...]
    pl.semaphore_wait(barrier, total)
    index = 0
    copies = []
    for r, peers in enumerate(rounds):
        batch = []
        for dp, cp in peers:
            batch.append((index, pltpu.make_async_remote_copy(
                src_ref=cur.at[r], dst_ref=slots.at[index], send_sem=send.at[index], recv_sem=recv.at[index],
                device_id={"dp": dp, "cp": cp}, device_id_type=MESH)))
            index += 1
        for _, copy in batch:
            copy.start()
        value = cur[r]
        for i, copy in batch:
            copy.wait_recv()
            value = jnp.maximum(value, slots[i])
        if r + 1 < len(rounds):
            cur[r + 1] = value
        else:
            best[...] = value
        copies += batch
    for _, copy in copies:
        copy.wait_send()


def global_peak(peak, sizes):
    n_copies = sum(n - 1 for n in sizes)
    vmem = pl.BlockSpec(memory_space=pltpu.VMEM)
    shape = peak.shape
    return pl.pallas_call(
        functools.partial(peak_kernel, sizes),
        name="global_peak",
        out_shape=jax.ShapeDtypeStruct(shape, F32),
        in_specs=[vmem], out_specs=vmem,
        scratch_shapes=[pltpu.VMEM((2,) + shape, F32), pltpu.VMEM((n_copies,) + shape, F32),
                        pltpu.SemaphoreType.DMA((n_copies,)), pltpu.SemaphoreType.DMA((n_copies,))],
        compiler_params=pltpu.CompilerParams(collective_id=1, has_side_effects=True),
        cost_estimate=pl.CostEstimate(flops=10_000_000, bytes_accessed=8192, transcendentals=0),
    )(peak)


def clip_kernel(best, w_q, w_k, q_new, k_new):
    factor = jnp.where(best[...] > TAU_CLIP, jnp.sqrt(TAU_CLIP / best[...]), 1.0)
    for h in range(2 * HEADS):
        cols = pl.ds(h * HEAD_DIM, HEAD_DIM)
        q_new[:, cols] = (w_q[:, cols].astype(F32) * factor[h:h + 1, :]).astype(BF16)
        k_new[:, cols] = (w_k[:, cols].astype(F32) * factor[h:h + 1, :]).astype(BF16)


def clip_weights(best, w_q, w_k):
    block = pl.BlockSpec((256, MODEL), lambda i: (i, 0))
    return pl.pallas_call(
        clip_kernel,
        name="clip",
        grid=(MODEL // 256,),
        out_shape=[jax.ShapeDtypeStruct(w_q.shape, BF16)] * 2,
        in_specs=[pl.BlockSpec(best.shape, lambda i: (0, 0)), block, block],
        out_specs=[block, block],
        cost_estimate=pl.CostEstimate(flops=1_000_000_000, bytes_accessed=4 * MODEL * MODEL * 2, transcendentals=0),
    )(best, w_q, w_k)


def solution(mesh):
    cp_size, dp_size = mesh.shape["cp"], mesh.shape["dp"]
    sizes = (dp_size // 8, 4)
    swap = []
    for quad in range(dp_size // 2):
        for x in range(cp_size):
            src_dp = 2 * quad + 1 - x // 2
            dst_x = cp_size - 1 - x
            dst_dp = 2 * quad + 1 - dst_x // 2
            swap.append((src_dp * cp_size + x, dst_dp * cp_size + dst_x))
            home = (2 * quad + x // 2) * cp_size + x
            swap.append((home, home))

    def device_body(hidden, pos_ids, w_q, w_k, w_v, w_o):
        inv_freq = ROPE_THETA ** (-np.arange(HEAD_DIM // 2) * (2.0 / HEAD_DIM))
        freq = jnp.asarray(np.concatenate([inv_freq, inv_freq])[None, :], F32)
        out, peak = attend(hidden[0], pos_ids.reshape(4, 128), freq, w_q, w_k, w_v, w_o)
        swapped = lax.ppermute(out, ("dp", "cp"), swap)
        best = global_peak(peak, sizes)
        w_q_new, w_k_new = clip_weights(best, w_q, w_k)
        return swapped[None], best[:, 0], w_q_new, w_k_new

    return jax.shard_map(
        device_body,
        mesh=mesh,
        in_specs=(P("dp", "cp", None), P("cp"), P(None, None), P(None, None), P(None, None), P(None, None)),
        out_specs=(P("dp", "cp", None), P(None), P(None, None), P(None, None)),
        check_vma=False,
    )
```

```python
import functools

import jax
import jax.numpy as jnp
import numpy as np
from jax import lax
from jax.experimental import pallas as pl
from jax.experimental.pallas import tpu as pltpu
from jax.sharding import PartitionSpec as P

HEAD_DIM = 128
TAU_CLIP = 100.0
ROPE_THETA = 50000.0
SCALE = HEAD_DIM ** -0.5
LOG2E = 1.4426950408889634
MESH = pl.DeviceIdType.MESH

PIECE = 512
HALF = 256
MODEL = 2048
COLS = 1024
HEADS = 8
OWN, FAR, NEAR, LAST = 0, 1, 2, 3
TABLE_OF = (0, 1, 2, 0)
F32, BF16 = jnp.float32, jnp.bfloat16


def attend_kernel(hid, pos, freq, w_q, w_k, w_v, w_o, out, peak,
                  hbuf, wk, wv, w_pair, qbuf, kbuf, vbuf, acc, run_max, run_sum, cos_t, sin_t, pos_all,
                  bias, top_all, wsem, send, recv, psend, precv, osem, tsend, trecv):
    x = lax.axis_index("cp")
    d = lax.axis_index("dp")
    core = lax.rem(d, 2)
    home = core == x // 2
    away = core != x // 2
    partner = d + 1 - 2 * core
    pair = x + 1 - 2 * lax.rem(x, 2)
    far_x = 3 - x
    piece_of = (x, far_x, pair, 3 - pair)
    col0 = pl.multiple_of(core * COLS, COLS)

    def rows(kind, half):
        return pl.ds(pl.multiple_of(piece_of[kind] * PIECE + half * HALF, HALF), HALF)

    def remote(src, dst, s_sem, r_sem, dp, cp):
        return pltpu.make_async_remote_copy(src_ref=src, dst_ref=dst, send_sem=s_sem, recv_sem=r_sem,
                                            device_id={"dp": dp, "cp": cp}, device_id_type=MESH)

    w_copies = [pltpu.make_async_copy(src.at[:, pl.ds(col0, COLS)], dst, wsem.at[i])
                for i, (src, dst) in enumerate(((w_k, wk), (w_v, wv), (w_q, w_pair.at[0])))]
    w_copies.append(pltpu.make_async_copy(w_o.at[:, pl.ds(COLS, COLS)], w_pair.at[1], wsem.at[3]))
    wo_low = pltpu.make_async_copy(w_o.at[:, pl.ds(0, COLS)], w_pair.at[0], wsem.at[6])

    def half_rows(j):
        return pl.ds(pl.multiple_of(j * HALF, HALF), HALF)

    def own_local(j):
        return pltpu.make_async_copy(hid.at[half_rows(j), :], hbuf.at[rows(OWN, j), :], wsem.at[4 + j])

    @pl.when(home)
    def _():
        for j in range(2):
            own_local(j).start()
    for copy in w_copies:
        copy.start()

    barrier = pltpu.get_barrier_semaphore()
    for k in range(1, 4):
        pl.semaphore_signal(barrier, inc=1, device_id={"dp": d, "cp": lax.rem(x + k, 4)}, device_id_type=MESH)
    pl.semaphore_signal(barrier, inc=1, device_id={"dp": partner, "cp": x}, device_id_type=MESH)
    pl.semaphore_wait(barrier, 4)

    def own_copy(j, to_pair):
        src = hid.at[half_rows(j), :]
        dst = hbuf.at[rows(OWN, j), :]
        if to_pair:
            return remote(src, dst, send.at[j], recv.at[NEAR * 2 + j], d, pair)
        return remote(src, dst, send.at[2 + j], recv.at[OWN * 2 + j], partner, x)

    def away_copy(j):
        return remote(hid.at[half_rows(j), :], hbuf.at[rows(OWN, j), :], send.at[12 + j], recv.at[FAR * 2 + j], d, far_x)

    def far_to_pair(j):
        return remote(hbuf.at[rows(FAR, j), :], hbuf.at[rows(FAR, j), :], send.at[4 + j], recv.at[LAST * 2 + j], d, pair)

    def to_partner(kind, j):
        return remote(hbuf.at[rows(kind, j), :], hbuf.at[rows(kind, j), :], send.at[4 + 2 * kind + j], recv.at[kind * 2 + j], partner, x)

    pos_copies = [remote(pos, pos_all.at[x], psend.at[k - 1], precv.at[k - 1], d, lax.rem(x + k, 4)) for k in range(1, 4)]
    for copy in pos_copies:
        copy.start()

    @pl.when(home)
    def _():
        @pl.when(x != 3)
        def _():
            for j in range(2):
                own_copy(j, True).start()
        for j in range(2):
            own_copy(j, False).start()

    @pl.when(away)
    def _():
        for j in range(2):
            away_copy(j).start()

    def tables(kind):
        piece = piece_of[kind]
        row_i = lax.broadcasted_iota(jnp.int32, (64, 128), 0)
        col_i = lax.broadcasted_iota(jnp.int32, (64, 128), 1)
        low = col_i < 64

        def one(b):
            if kind == OWN:
                line = pos[pl.ds(b, 1), :]
            else:
                line = pos_all[pl.ds(piece, 1), pl.ds(b, 1), :].reshape(1, 128)
            line = jnp.broadcast_to(line.astype(F32), (64, 128))
            first = jnp.sum(jnp.where(row_i == col_i, line, 0.0), axis=1, keepdims=True)
            second = jnp.sum(jnp.where(row_i + 64 == col_i, line, 0.0), axis=1, keepdims=True)
            angle = jnp.where(low, first, second) * freq[...]
            cos_a, sin_a = jnp.cos(angle), jnp.sin(angle)
            cos_r, sin_r = pltpu.roll(cos_a, 64, 1), pltpu.roll(sin_a, 64, 1)
            at = pl.multiple_of(TABLE_OF[kind] * PIECE + b * 128, 128)
            cos_t[pl.ds(at, 64), :] = jnp.where(low, cos_a, cos_r)
            cos_t[pl.ds(at + 64, 64), :] = jnp.where(low, cos_r, cos_a)
            sin_t[pl.ds(at, 64), :] = jnp.where(low, -sin_a, sin_r)
            sin_t[pl.ds(at + 64, 64), :] = jnp.where(low, -sin_r, sin_a)

        def block(b, carry):
            one(2 * b)
            one(2 * b + 1)
            return carry

        lax.fori_loop(0, 2, block, 0)

    def rotate(t, cos_v, sin_v):
        parts = []
        for h in range(HEADS):
            u = t[:, h * HEAD_DIM:(h + 1) * HEAD_DIM]
            parts.append((u * cos_v + pltpu.roll(u, 64, 1) * sin_v).astype(BF16))
        return jnp.concatenate(parts, axis=1)

    def project(kind, half, with_q):
        at = rows(kind, half)
        table = pl.ds(pl.multiple_of(TABLE_OF[kind] * PIECE + half * HALF, HALF), HALF)
        cos_v, sin_v = cos_t[table, :], sin_t[table, :]
        h = hbuf[at, :]
        kbuf[at, :] = rotate(jnp.dot(h, wk[...], preferred_element_type=F32), cos_v, sin_v)
        vbuf[at, :] = jnp.dot(h, wv[...], preferred_element_type=F32).astype(BF16)
        if with_q:
            q_at = pl.ds(pl.multiple_of(half * HALF, HALF), HALF)
            qbuf[kind, q_at, :] = rotate(jnp.dot(h, w_pair[0], preferred_element_type=F32), cos_v, sin_v)

    def tile(slot, piece, diagonal):
        key0 = pl.multiple_of(piece * PIECE, PIECE)
        units = [(h, qb) for h in range(HEADS) for qb in range(2)]

        def scores(h, qb):
            n_keys = HALF * (qb + 1) if diagonal else PIECE
            cols = pl.ds(h * HEAD_DIM, HEAD_DIM)
            s = lax.dot_general(qbuf[slot, pl.ds(qb * HALF, HALF), cols], kbuf[pl.ds(key0, n_keys), cols],
                                (((1,), (1,)), ((), ())), preferred_element_type=F32)
            if diagonal:
                last = s[:, n_keys - HALF:] + bias[...]
                s = last if qb == 0 else jnp.concatenate([s[:, :n_keys - HALF], last], axis=1)
            return s

        results = []
        s = scores(*units[0])
        for i, (h, qb) in enumerate(units):
            s_next = scores(*units[i + 1]) if i + 1 < len(units) else None
            at = pl.ds(qb * HALF, HALF)
            n_keys = s.shape[1]
            top = jnp.max(s, axis=1, keepdims=True)
            old = None if diagonal else run_max[slot, h, at, :]
            new = jnp.broadcast_to(top, (HALF, 128)) if diagonal else jnp.maximum(old, top)
            p = jnp.exp2((s - jnp.concatenate([new] * (n_keys // 128), axis=1)) * (SCALE * LOG2E))
            total = p[:, :128]
            for g in range(1, n_keys // 128):
                total = total + p[:, g * 128:(g + 1) * 128]
            part = jnp.dot(p.astype(BF16), vbuf[pl.ds(key0, n_keys), pl.ds(h * HEAD_DIM, HEAD_DIM)],
                           preferred_element_type=F32)
            results.append((old, new, total, part))
            s = s_next
        for (h, qb), (old, new, total, part) in zip(units, results):
            at, cols = pl.ds(qb * HALF, HALF), pl.ds(h * HEAD_DIM, HEAD_DIM)
            if not diagonal:
                fade = jnp.exp2((old - new) * (SCALE * LOG2E))
                total = total + run_sum[slot, h, at, :] * fade
                part = part + acc[slot, at, cols] * fade
            run_max[slot, h, at, :] = new
            run_sum[slot, h, at, :] = total
            acc[slot, at, cols] = part

    def arrive(kind, j):
        @pl.when(home)
        def _():
            if kind == OWN:
                own_local(j).wait()
            else:
                away_copy(j).wait_recv() if kind == FAR else own_copy(j, True).wait_recv() if kind == NEAR else far_to_pair(j).wait_recv()
                if kind == FAR:
                    @pl.when(x != 0)
                    def _():
                        far_to_pair(j).start()
                to_partner(kind, j).start()

        @pl.when(away)
        def _():
            if kind == OWN:
                own_copy(j, False).wait_recv()
            else:
                to_partner(kind, j).wait_recv()

    bias[...] = jnp.where(lax.broadcasted_iota(jnp.int32, (HALF, HALF), 0) >= lax.broadcasted_iota(jnp.int32, (HALF, HALF), 1),
                          0.0, -jnp.inf)
    tables(OWN)
    for copy in pos_copies:
        copy.wait_recv()
    tables(FAR)
    tables(NEAR)
    for i in range(3):
        w_copies[i].wait()

    def own_half(j, carry):
        arrive(OWN, j)
        project(OWN, j, True)
        return carry

    lax.fori_loop(0, 2, own_half, 0)
    @pl.when(x >= 0)
    def _():
        tile(OWN, x, True)


    def far_half(j, carry):
        arrive(FAR, j)

        @pl.when(x != 2)
        def _():
            arrive(NEAR, j)

        project(FAR, j, True)

        @pl.when(x != 2)
        def _():
            project(NEAR, j, False)
        return carry

    lax.fori_loop(0, 2, far_half, 0)
    wo_low.start()
    tables(LAST)

    @pl.when(x >= 0)
    def _():
        tile(FAR, far_x, True)

    later = jnp.where(x < 2, FAR, OWN)

    def near_tile(i, carry):
        slot = jnp.where(i == 0, later, i - 1)
        piece = jnp.where(i == 0, jnp.minimum(x, far_x), pair)

        @pl.when((i == 0) | ((i == 1) & (lax.rem(x, 2) == 1)) | ((i == 2) & (x < 2)))
        def _():
            tile(slot, piece, False)
        return carry

    lax.fori_loop(0, 3, near_tile, 0)

    early = 1 - later
    mine = jnp.where(core == 0, early, later)
    exchange = remote(qbuf.at[1 - mine], qbuf.at[2], osem.at[0], osem.at[1], partner, x)
    own_rows = pl.ds(pl.multiple_of(x * PIECE, PIECE), PIECE)

    def out_copy(part):
        cols = pl.ds(pl.multiple_of(part * COLS, COLS), COLS)
        return pltpu.make_async_copy(hbuf.at[own_rows, cols], out.at[:, cols], wsem.at[7 + part])

    def finish(slot):
        for h in range(HEADS):
            cols = pl.ds(h * HEAD_DIM, HEAD_DIM)
            total = jnp.sum(run_sum[slot, h, :, :], axis=1, keepdims=True)
            qbuf[slot, :, cols] = (acc[slot, :, cols] / total).astype(BF16)

    def output(part):
        heads = jnp.concatenate([qbuf[jnp.where(core == 0, mine, 2)], qbuf[jnp.where(core == 0, 2, mine)]], axis=1)
        value = jnp.dot(heads, w_pair[part], preferred_element_type=F32)
        hbuf[own_rows, pl.ds(pl.multiple_of(part * COLS, COLS), COLS)] = value.astype(BF16)
        out_copy(part).start()

    outer = (x == 0) | (x == 3)

    @pl.when(outer)
    def _():
        finish(early)

        @pl.when(core == 1)
        def _():
            exchange.start()

    @pl.when(x != 1)
    def _():
        def last_half(j, carry):
            arrive(LAST, j)
            project(LAST, j, False)
            return carry
        lax.fori_loop(0, 2, last_half, 0)

    def last_tile(slot, carry):
        @pl.when(((slot == OWN) & (x >= 2)) | ((slot == FAR) & (lax.rem(x, 2) == 0)))
        def _():
            tile(slot, 3 - pair, False)
        return carry

    lax.fori_loop(0, 2, last_tile, 0)

    finish(later)

    @pl.when(core == 0)
    def _():
        exchange.start()

    top_all[0] = jnp.full((2 * HEADS, 128), -jnp.inf, F32)
    for h in range(HEADS):
        top = jnp.maximum(jnp.max(run_max[0, h, :, :], axis=0, keepdims=True), jnp.max(run_max[1, h, :, :], axis=0, keepdims=True))
        top_all[0, pl.ds(core * HEADS + h, 1), :] = top * SCALE
    top_copies = [remote(top_all.at[0], top_all.at[k], tsend.at[k - 1], trecv.at[k - 1], d, lax.rem(x + k, 4)) for k in range(1, 4)]
    top_copies.append(remote(top_all.at[4], top_all.at[5], tsend.at[3], trecv.at[3], partner, x))
    for copy in top_copies[:3]:
        copy.start()

    @pl.when(jnp.logical_not(outer))
    def _():
        finish(early)

        @pl.when(core == 1)
        def _():
            exchange.start()

    w_copies[3].wait()
    wo_low.wait()
    exchange.wait_recv()

    @pl.when(x >= 0)
    def _():
        output(0)

    best = top_all[0]
    for k in range(3):
        top_copies[k].wait_recv()
        best = jnp.maximum(best, top_all[k + 1])
    top_all[4] = best
    top_copies[3].start()

    @pl.when(x >= 0)
    def _():
        output(1)

    top_copies[3].wait_recv()
    peak[...] = jnp.maximum(top_all[4], top_all[5])
    for copy in top_copies:
        copy.wait_send()
    for part in range(2):
        out_copy(part).wait()

    exchange.wait_send()
    for copy in pos_copies:
        copy.wait_send()

    @pl.when(away)
    def _():
        for j in range(2):
            away_copy(j).wait_send()

    @pl.when(home)
    def _():
        for j in range(2):
            own_copy(j, False).wait_send()
            to_partner(FAR, j).wait_send()

        @pl.when(x != 3)
        def _():
            for j in range(2):
                own_copy(j, True).wait_send()

        @pl.when(x != 0)
        def _():
            for j in range(2):
                far_to_pair(j).wait_send()

        @pl.when(x != 2)
        def _():
            for j in range(2):
                to_partner(NEAR, j).wait_send()

        @pl.when(x != 1)
        def _():
            for j in range(2):
                to_partner(LAST, j).wait_send()


def attend(hid, pos, freq, w_q, w_k, w_v, w_o):
    any_spec = pl.BlockSpec(memory_space=pl.ANY)
    vmem = pl.BlockSpec(memory_space=pltpu.VMEM)
    return pl.pallas_call(
        attend_kernel,
        name="attend",
        out_shape=[jax.ShapeDtypeStruct((PIECE, MODEL), BF16), jax.ShapeDtypeStruct((2 * HEADS, 128), F32)],
        in_specs=[any_spec, vmem, vmem, any_spec, any_spec, any_spec, any_spec],
        out_specs=[any_spec, vmem],
        scratch_shapes=[
            pltpu.VMEM((4 * PIECE, MODEL), BF16),
            pltpu.VMEM((MODEL, COLS), BF16), pltpu.VMEM((MODEL, COLS), BF16), pltpu.VMEM((2, MODEL, COLS), BF16),
            pltpu.VMEM((3, PIECE, COLS), BF16), pltpu.VMEM((4 * PIECE, COLS), BF16), pltpu.VMEM((4 * PIECE, COLS), BF16),
            pltpu.VMEM((2, PIECE, COLS), F32), pltpu.VMEM((2, HEADS, PIECE, 128), F32), pltpu.VMEM((2, HEADS, PIECE, 128), F32),
            pltpu.VMEM((3 * PIECE, 128), F32), pltpu.VMEM((3 * PIECE, 128), F32), pltpu.VMEM((4, 4, 128), jnp.int32),
            pltpu.VMEM((HALF, HALF), F32), pltpu.VMEM((6, 2 * HEADS, 128), F32),
            pltpu.SemaphoreType.DMA((9,)), pltpu.SemaphoreType.DMA((14,)), pltpu.SemaphoreType.DMA((8,)),
            pltpu.SemaphoreType.DMA((3,)), pltpu.SemaphoreType.DMA((3,)), pltpu.SemaphoreType.DMA((2,)),
            pltpu.SemaphoreType.DMA((4,)), pltpu.SemaphoreType.DMA((4,)),
        ],
        compiler_params=pltpu.CompilerParams(collective_id=0, has_side_effects=True, vmem_limit_bytes=67043328),
        cost_estimate=pl.CostEstimate(flops=31_000_000_000, bytes_accessed=26_000_000, transcendentals=11_000_000),
    )(hid, pos, freq, w_q, w_k, w_v, w_o)


def peak_kernel(sizes, peak, best, cur, slots, send, recv):
    n_z, n_y = sizes
    x = lax.axis_index("cp")
    d = lax.axis_index("dp")
    core, y, z = lax.rem(d, 2), lax.rem(d // 2, n_y), d // (2 * n_y)
    rounds = [
        [((z * n_y + lax.rem(y + k, n_y)) * 2 + core, x) for k in range(1, n_y)],
        [((lax.rem(z + k, n_z) * n_y + y) * 2 + core, x) for k in range(1, n_z)],
    ]
    barrier = pltpu.get_barrier_semaphore()
    total = 0
    for peers in rounds:
        for dp, cp in peers:
            pl.semaphore_signal(barrier, inc=1, device_id={"dp": dp, "cp": cp}, device_id_type=MESH)
            total += 1
    cur[0] = peak[...]
    pl.semaphore_wait(barrier, total)
    index = 0
    copies = []
    for r, peers in enumerate(rounds):
        batch = []
        for dp, cp in peers:
            batch.append((index, pltpu.make_async_remote_copy(
                src_ref=cur.at[r], dst_ref=slots.at[index], send_sem=send.at[index], recv_sem=recv.at[index],
                device_id={"dp": dp, "cp": cp}, device_id_type=MESH)))
            index += 1
        for _, copy in batch:
            copy.start()
        value = cur[r]
        for i, copy in batch:
            copy.wait_recv()
            value = jnp.maximum(value, slots[i])
        if r + 1 < len(rounds):
            cur[r + 1] = value
        else:
            best[...] = value
        copies += batch
    for _, copy in copies:
        copy.wait_send()


def global_peak(peak, sizes):
    n_copies = sum(n - 1 for n in sizes)
    vmem = pl.BlockSpec(memory_space=pltpu.VMEM)
    shape = peak.shape
    return pl.pallas_call(
        functools.partial(peak_kernel, sizes),
        name="global_peak",
        out_shape=jax.ShapeDtypeStruct(shape, F32),
        in_specs=[vmem], out_specs=vmem,
        scratch_shapes=[pltpu.VMEM((2,) + shape, F32), pltpu.VMEM((n_copies,) + shape, F32),
                        pltpu.SemaphoreType.DMA((n_copies,)), pltpu.SemaphoreType.DMA((n_copies,))],
        compiler_params=pltpu.CompilerParams(collective_id=1, has_side_effects=True),
        cost_estimate=pl.CostEstimate(flops=10_000_000, bytes_accessed=8192, transcendentals=0),
    )(peak)


def clip_weights(head_max, w_q, w_k):
    factor = jnp.where(head_max > TAU_CLIP, jnp.sqrt(TAU_CLIP / head_max), 1.0)
    col_factor = jnp.repeat(factor, HEAD_DIM)[None, :]
    return (w_q.astype(F32) * col_factor).astype(BF16), (w_k.astype(F32) * col_factor).astype(BF16)


def solution(mesh):
    cp_size, dp_size = mesh.shape["cp"], mesh.shape["dp"]
    sizes = (dp_size // 8, 4)
    swap = []
    for quad in range(dp_size // 2):
        for x in range(cp_size):
            src_dp = 2 * quad + 1 - x // 2
            dst_x = cp_size - 1 - x
            dst_dp = 2 * quad + 1 - dst_x // 2
            swap.append((src_dp * cp_size + x, dst_dp * cp_size + dst_x))
            home = (2 * quad + x // 2) * cp_size + x
            swap.append((home, home))

    def device_body(hidden, pos_ids, w_q, w_k, w_v, w_o):
        inv_freq = ROPE_THETA ** (-np.arange(HEAD_DIM // 2) * (2.0 / HEAD_DIM))
        freq = jnp.asarray(np.concatenate([inv_freq, inv_freq])[None, :], F32)
        out, peak = attend(hidden[0], pos_ids.reshape(4, 128), freq, w_q, w_k, w_v, w_o)
        swapped = lax.ppermute(out, ("dp", "cp"), swap)
        head_max = global_peak(peak, sizes)[:, 0]
        w_q_new, w_k_new = clip_weights(head_max, w_q, w_k)
        return swapped[None], head_max, w_q_new, w_k_new

    return jax.shard_map(
        device_body,
        mesh=mesh,
        in_specs=(P("dp", "cp", None), P("cp"), P(None, None), P(None, None), P(None, None), P(None, None)),
        out_specs=(P("dp", "cp", None), P(None), P(None, None), P(None, None)),
        check_vma=False,
    )
```
